8 devices in a mesh: dp: 1 (over z), ri: 2 (over y), co: 2 (over x), ro: 2 (over core).
Axes of the slice: x: 2, y: 2, z: 1, core: 2. Of those that a mesh axis runs over, the one named last changes fastest.
Arguments:
- act_in: bfloat16 [8192, 2048], P(('dp', 'ro', 'ri'), 'co')
- weight: bfloat16 [2048, 8192], P(('ro', 'ri'), 'co')
Outputs:
- output: bfloat16 [8192, 8192], P(('dp', 'ro', 'ri', 'co'))
All inputs are finite; a program needn't handle non-finite values.
Results may differ from the reference program's by a relative error of at most 0.001.
Values are sent between devices in bfloat16 or wider.
A program may use at most 1 GiB of HBM per device.

```python
import jax
import jax.numpy as jnp

ROWS_TOTAL = 8192
D_IN = 2048
D_OUT = 8192


def setup_inputs(seed: int = 0, part: int = 0) -> dict:
    key = jax.random.key(seed)
    key_a = jax.random.fold_in(jax.random.fold_in(key, 1), part)
    key_b = jax.random.fold_in(key, 2)
    act_in = jax.random.normal(key_a, (ROWS_TOTAL, D_IN), jnp.float32)
    weight = jax.random.normal(key_b, (D_IN, D_OUT), jnp.float32) * (D_IN ** -0.5)
    return {"act_in": act_in.astype(jnp.bfloat16), "weight": weight.astype(jnp.bfloat16)}


def reference(act_in, weight):
    product = jnp.dot(act_in, weight, preferred_element_type=jnp.float32)
    return product.astype(jnp.bfloat16)
```

```python
import jax
import jax.numpy as jnp
from jax import lax
from jax.experimental import pallas as pl
from jax.experimental.pallas import tpu as pltpu
from jax.sharding import PartitionSpec as P

MESH = pl.DeviceIdType.MESH
W = 256
VIA_X = 4


def _kernel(a_ref, b_ref, o_ref, abuf, bbuf, cbuf, x_send, x_recv, y_send, y_recv, p_send, p_recv, a_sem, l_sem, o_sem):
    ri, co, ro = lax.axis_index("ri"), lax.axis_index("co"), lax.axis_index("ro")
    to_x, to_y, to_p = {"co": 1 - co}, {"ri": 1 - ri}, {"ro": 1 - ro}
    depth, half = b_ref.shape
    rows, k_half = a_ref.shape[0] // 2, a_ref.shape[1]
    n = half // W
    via_y = n - VIA_X

    mine = pl.ds(pl.multiple_of((ro * 2 + ri) * depth, depth), depth)
    other = pl.ds(pl.multiple_of((ro * 2 + 1 - ri) * depth, depth), depth)

    def remote(src, dst, sems, i, to):
        return pltpu.make_async_remote_copy(
            src_ref=src, dst_ref=dst, send_sem=sems[0].at[i], recv_sem=sems[1].at[i], device_id=to, device_id_type=MESH
        )

    xs, ys, ps = (x_send, x_recv), (y_send, y_recv), (p_send, p_recv)
    a_cols = pl.ds(pl.multiple_of(co * k_half, k_half), k_half)

    def own(s):
        return b_ref.at[:, pl.ds(pl.multiple_of(s * W, W), W)]

    a_out = remote(a_ref.at[pl.ds(pl.multiple_of((1 - co) * rows, rows), rows), :], abuf.at[:, a_cols], xs, 0, to_x)
    a_loc = pltpu.make_async_copy(a_ref.at[pl.ds(pl.multiple_of(co * rows, rows), rows), :], abuf.at[:, a_cols], a_sem)
    x_own = lambda s: remote(own(s), bbuf.at[1, s, mine, :], xs, 1 + s, to_x)
    y_own = lambda s: remote(own(s), bbuf.at[0, s, mine, :], ys, s, to_y)
    p_own = lambda s: remote(own(s), bbuf.at[0, s, mine, :], ps, s, to_p)
    l_own = lambda s: pltpu.make_async_copy(own(s), bbuf.at[0, s, mine, :], l_sem.at[s])
    p_y = lambda s: remote(bbuf.at[0, s, other, :], bbuf.at[0, s, other, :], ps, n + s, to_p)
    p_x = lambda s: remote(bbuf.at[1, s, mine, :], bbuf.at[1, s, mine, :], ps, 2 * n + s, to_p)
    p_d = lambda s: remote(bbuf.at[1, s, other, :], bbuf.at[1, s, other, :], ps, 3 * n + s, to_p)
    x_rel = lambda s: remote(bbuf.at[0, s, other, :], bbuf.at[1, s, other, :], xs, 1 + n + s - via_y, to_x)
    y_rel = lambda s: remote(bbuf.at[1, s, mine, :], bbuf.at[1, s, mine, :], ys, n + s, to_y)

    def out(h, s, slot):
        col = (co if h == 0 else 1 - co) * half + s * W
        return pltpu.make_async_copy(cbuf.at[slot], o_ref.at[:, pl.ds(pl.multiple_of(col, W), W)], o_sem.at[slot])

    barrier = pltpu.get_barrier_semaphore()
    for to in (to_x, to_y, to_p):
        pl.semaphore_signal(barrier, inc=1, device_id=to, device_id_type=MESH)
    pl.semaphore_wait(barrier, 3)

    a_out.start()

    @pl.loop(0, n)
    def _(s):
        x_own(s).start()
        y_own(s).start()

    a_loc.start()

    @pl.loop(0, n)
    def _(s):
        l_own(s).start()
        p_own(s).start()

    def compute(h, s, step):
        slot = lax.rem(step, 2)
        if h == 0:
            l_own(s).wait()
            p_own(s).wait_recv()
            p_y(s).wait_recv()
        else:
            p_x(s).wait_recv()
            p_d(s).wait_recv()

        @pl.when(step >= 2)
        def _():
            out(h, s, slot).wait()

        @pl.loop(0, 2)
        def _(r):
            block = pl.ds(pl.multiple_of(r * (rows // 2), rows // 2), rows // 2)
            c = jnp.dot(abuf[block, :], bbuf[h, s], preferred_element_type=jnp.float32)
            cbuf[slot, block, :] = c.astype(cbuf.dtype)

        out(h, s, slot).start()

    head = n - 8

    @pl.loop(0, head)
    def _(t):
        y_own(t).wait_recv()
        p_y(t).start()

    a_loc.wait()
    a_out.wait_recv()

    @pl.loop(head, n)
    def _(t):
        y_own(t).wait_recv()
        p_y(t).start()

        @pl.when(t >= via_y)
        def _():
            x_rel(t).start()

        s = t - head
        x_own(s).wait_recv()
        p_x(s).start()
        y_rel(s).start()

        @pl.loop(0, 2)
        def _(i):
            compute(0, 2 * s + i, 2 * s + i)

    @pl.loop(0, n - 8)
    def _(m):
        y_rel(m).wait_recv()
        p_d(m).start()
        s = m + 8
        x_own(s).wait_recv()
        p_x(s).start()

        @pl.when(s < via_y)
        def _():
            y_rel(s).start()

        compute(1, m, n + m)

    @pl.loop(0, VIA_X)
    def _(i):
        m, s = n - 8 + i, via_y + i
        y_rel(m).wait_recv()
        p_d(m).start()
        x_rel(s).wait_recv()
        p_d(s).start()

        @pl.loop(0, 2)
        def _(j):
            compute(1, m + j * VIA_X, 2 * n - 8 + 2 * i + j)

    a_out.wait_send()

    @pl.loop(0, n)
    def _(s):
        x_own(s).wait_send()
        y_own(s).wait_send()
        p_own(s).wait_send()
        p_y(s).wait_send()
        p_x(s).wait_send()
        p_d(s).wait_send()

    @pl.loop(0, via_y)
    def _(s):
        y_rel(s).wait_send()

    @pl.loop(via_y, n)
    def _(s):
        x_rel(s).wait_send()

    out(1, 0, 0).wait()
    out(1, 0, 1).wait()


def solution(mesh):
    def local_block(act_blk, weight_blk):
        rows, k = act_blk.shape[0] // 2, act_blk.shape[1] * 2
        half = weight_blk.shape[1]
        n = half // W
        via_y = n - VIA_X
        return pl.pallas_call(
            _kernel,
            out_shape=jax.ShapeDtypeStruct((rows, 2 * half), jnp.bfloat16),
            in_specs=[pl.BlockSpec(memory_space=pl.ANY)] * 2,
            out_specs=pl.BlockSpec(memory_space=pl.ANY),
            scratch_shapes=[
                pltpu.VMEM((rows, k), jnp.bfloat16),
                pltpu.VMEM((2, n, k, W), jnp.bfloat16),
                pltpu.VMEM((2, rows, W), jnp.bfloat16),
                pltpu.SemaphoreType.DMA((1 + n + VIA_X,)),
                pltpu.SemaphoreType.DMA((1 + n + VIA_X,)),
                pltpu.SemaphoreType.DMA((n + via_y,)),
                pltpu.SemaphoreType.DMA((n + via_y,)),
                pltpu.SemaphoreType.DMA((4 * n,)),
                pltpu.SemaphoreType.DMA((4 * n,)),
                pltpu.SemaphoreType.DMA,
                pltpu.SemaphoreType.DMA((n,)),
                pltpu.SemaphoreType.DMA((2,)),
            ],
            compiler_params=pltpu.CompilerParams(collective_id=0, has_side_effects=True),
        )(act_blk, weight_blk)

    return jax.shard_map(
        local_block,
        mesh=mesh,
        in_specs=(P(("dp", "ro", "ri"), "co"), P(("ro", "ri"), "co")),
        out_specs=P(("dp", "ro", "ri", "co"), None),
        check_vma=False,
    )
```

```python
import jax
import jax.numpy as jnp
from jax import lax
from jax.experimental import pallas as pl
from jax.experimental.pallas import tpu as pltpu
from jax.sharding import PartitionSpec as P

MESH = pl.DeviceIdType.MESH
W = 256
ROWS = 128
OWN = ((0, 1024), (1024, 1024), (2048, 512), (3328, 768), (2560, 768))
VIA_Y = (
    (0, 1024, 0),
    (1024, 512, 1),
    (1536, 512, 1),
    (2048, 256, 2),
    (2304, 256, 2),
    (3328, 256, 3),
    (3584, 128, 3),
    (3712, 128, 3),
)
VIA_X = ((2560, 256, 4), (2816, 256, 4), (3072, 256, 4), (3840, 128, 4), (3968, 128, 4))
LAST = 3328


def _gather(a_ref, b_ref, abuf, bbuf, c_ref, x_send, y_send, p_send, x_recv, y_recv, p_recv, l_sem):
    ri, co, ro = lax.axis_index("ri"), lax.axis_index("co"), lax.axis_index("ro")
    to_x, to_y, to_p = {"co": 1 - co}, {"ri": 1 - ri}, {"ro": 1 - ro}
    depth, half = b_ref.shape
    rows, k_half = a_ref.shape[0] // 2, a_ref.shape[1]

    mine = pl.ds(pl.multiple_of((ro * 2 + ri) * depth, depth), depth)
    other = pl.ds(pl.multiple_of((ro * 2 + 1 - ri) * depth, depth), depth)
    a_cols = pl.ds(pl.multiple_of(co * k_half, k_half), k_half)

    def remote(src, dst, send, recv, to):
        return pltpu.make_async_remote_copy(
            src_ref=src, dst_ref=dst, send_sem=send, recv_sem=recv, device_id=to, device_id_type=MESH
        )

    def over_x(src, dst, i):
        return remote(src, dst, x_send, x_recv.at[i], to_x)

    def over_y(src, dst, i):
        return remote(src, dst, y_send, y_recv.at[i], to_y)

    def over_p(src, dst, i):
        return remote(src, dst, p_send, p_recv.at[i], to_p)

    n = len(OWN)
    cut = lambda h, k_rows, piece: bbuf.at[h, k_rows, pl.ds(piece[0], piece[1])]
    own = [cut(0, mine, OWN[0])] + [b_ref.at[:, pl.ds(*piece)] for piece in OWN[1:]]
    a_out = over_x(a_ref.at[pl.ds(pl.multiple_of((1 - co) * rows, rows), rows), :], abuf.at[:, a_cols], 0)
    a_loc = pltpu.make_async_copy(
        a_ref.at[pl.ds(pl.multiple_of(co * rows, rows), rows), :], abuf.at[:, a_cols], l_sem.at[0]
    )
    first = OWN[0][1]
    b_first = pltpu.make_async_copy(b_ref.at[:, pl.ds(0, first)], cut(0, mine, OWN[0]), l_sem.at[1])
    rest = pl.ds(first, half - first)
    b_rest = pltpu.make_async_copy(b_ref.at[:, rest], bbuf.at[0, mine, rest], l_sem.at[2])
    x_own = [over_x(own[i], cut(1, mine, OWN[i]), 1 + i) for i in range(n)]
    y_own = [over_y(own[i], cut(0, mine, OWN[i]), i) for i in range(n)]
    x_rel = [over_x(cut(0, other, p), cut(1, other, p), 1 + n + i) for i, p in enumerate(VIA_X)]
    y_rel = [over_y(cut(1, mine, p), cut(1, mine, p), n + i) for i, p in enumerate(VIA_Y)]
    p_own = over_p(b_ref, bbuf.at[0, mine, :], 0)
    p_y = [over_p(cut(0, other, p), cut(0, other, p), 1 + i) for i, p in enumerate(OWN)]
    p_x = [over_p(cut(1, mine, p), cut(1, mine, p), 1 + n + i) for i, p in enumerate(OWN)]
    p_dy = [over_p(cut(1, other, p), cut(1, other, p), 1 + 2 * n + i) for i, p in enumerate(VIA_Y)]
    p_dx = [over_p(cut(1, other, p), cut(1, other, p), 1 + 2 * n + len(VIA_Y) + i) for i, p in enumerate(VIA_X)]

    barrier = pltpu.get_barrier_semaphore()
    for to in (to_x, to_y, to_p):
        pl.semaphore_signal(barrier, inc=1, device_id=to, device_id_type=MESH)
    b_first.start()
    pl.semaphore_wait(barrier, 3)

    b_first.wait()
    x_own[0].start()
    y_own[0].start()
    a_out.start()
    for i in range(1, n):
        y_own[i].start()
        x_own[i].start()
    b_rest.start()
    a_loc.start()
    p_own.start()

    def multiply(h, start, size):
        @pl.loop(0, size // W)
        def _(s):
            cols = pl.ds(pl.multiple_of(start + s * W, W), W)
            c = jnp.dot(abuf[...], bbuf[h, :, cols], preferred_element_type=jnp.float32)
            c_ref[h, :, cols] = c.astype(c_ref.dtype)

    def from_y(i):
        y_own[i].wait_recv()
        p_y[i].start()
        for j, p in enumerate(VIA_X):
            if p[2] == i:
                x_rel[j].start()

    def from_x(i):
        x_own[i].wait_recv()
        p_x[i].start()
        for j, p in enumerate(VIA_Y):
            if p[2] == i:
                y_rel[j].start()

    def own_half(i):
        p_y[i].wait_recv()
        multiply(0, *OWN[i])

    def diagonal(i):
        y_rel[i].wait_recv()
        p_dy[i].start()

    def diagonal_x(i):
        x_rel[i].wait_recv()
        p_dx[i].start()

    def multiply_y(i):
        p_dy[i].wait_recv()
        multiply(1, *VIA_Y[i][:2])

    def multiply_x(i):
        p_dx[i].wait_recv()
        multiply(1, *VIA_X[i][:2])

    from_y(0)
    from_x(0)
    from_y(1)
    from_y(2)
    from_y(3)
    a_loc.wait()
    b_rest.wait()
    p_own.wait_recv()
    a_out.wait_recv()
    for i in range(4):
        own_half(i)
    from_y(4)
    from_x(1)
    own_half(4)
    from_x(2)
    from_x(3)
    diagonal(0)
    for i in range(4):
        p_x[i].wait_recv()
    multiply_y(0)
    from_x(4)
    diagonal(1)
    diagonal(2)
    p_x[4].wait_recv()
    multiply_y(1)
    diagonal(3)
    diagonal_x(0)
    multiply_y(2)
    diagonal(4)
    diagonal_x(1)
    multiply_y(3)
    multiply_x(0)
    diagonal(5)
    diagonal_x(2)
    multiply_y(4)
    multiply_x(1)
    diagonal(6)
    diagonal_x(3)
    diagonal(7)
    diagonal_x(4)
    multiply_x(2)
    for copy in p_dy[5:] + p_dx[3:]:
        copy.wait_recv()

    link = bbuf.at[0, pl.ds(0, 7 * k_half // 8), :]
    remote(link, link, x_send, x_recv.at[0], to_x).wait_send()
    remote(link, link, y_send, y_recv.at[0], to_y).wait_send()
    remote(bbuf.at[0], bbuf.at[0], p_send, p_recv.at[0], to_p).wait_send()


def _write(abuf, bbuf, c_ref, o_ref, last, sem):
    co = lax.axis_index("co")
    rows, half = c_ref.shape[1:]
    n = rows // ROWS
    near = pl.multiple_of(co * half, half)
    far = pl.multiple_of((1 - co) * half, half)

    tail = half - LAST
    copies = []

    def write(src, block, cols):
        copies.append(pltpu.make_async_copy(src, o_ref.at[block, cols], sem.at[len(copies)]))
        copies[-1].start()

    blocks = [pl.ds(r * ROWS, ROWS) for r in range(n)]
    for block in blocks:
        write(c_ref.at[0, block, :], block, pl.ds(near, half))
        write(c_ref.at[1, block, pl.ds(0, LAST)], block, pl.ds(far, LAST))
    for block in blocks:
        c = jnp.dot(abuf[block, :], bbuf[1, :, LAST:], preferred_element_type=jnp.float32)
        last[block, :] = c.astype(last.dtype)
        write(last.at[block, :], block, pl.ds(pl.multiple_of(far + LAST, W), tail))
    for copy in copies:
        copy.wait()


def solution(mesh):
    def local_block(act_blk, weight_blk):
        rows, k = act_blk.shape[0] // 2, act_blk.shape[1] * 2
        half = weight_blk.shape[1]
        dma = pltpu.SemaphoreType.DMA
        vmem = pl.BlockSpec(memory_space=pltpu.VMEM)
        hbm = pl.BlockSpec(memory_space=pl.ANY)
        gathered = pl.pallas_call(
            _gather,
            out_shape=(
                pltpu.VMEM((rows, k), jnp.bfloat16),
                pltpu.VMEM((2, k, half), jnp.bfloat16),
                pltpu.VMEM((2, rows, half), jnp.bfloat16),
            ),
            in_specs=[hbm, hbm],
            out_specs=(vmem, vmem, vmem),
            scratch_shapes=[
                dma,
                dma,
                dma,
                dma((1 + len(OWN) + len(VIA_X),)),
                dma((len(OWN) + len(VIA_Y),)),
                dma((1 + 2 * len(OWN) + len(VIA_Y) + len(VIA_X),)),
                dma((3,)),
            ],
            compiler_params=pltpu.CompilerParams(
                collective_id=0, has_side_effects=True, vmem_limit_bytes=4 * 2**20
            ),
        )(
            pltpu.with_memory_space_constraint(act_blk, pltpu.HBM),
            pltpu.with_memory_space_constraint(weight_blk, pltpu.HBM),
        )
        return pl.pallas_call(
            _write,
            out_shape=jax.ShapeDtypeStruct((rows, 2 * half), jnp.bfloat16),
            in_specs=[vmem, vmem, vmem],
            out_specs=hbm,
            scratch_shapes=[pltpu.VMEM((rows, half - LAST), jnp.bfloat16), dma((3 * rows // ROWS,))],
            compiler_params=pltpu.CompilerParams(vmem_limit_bytes=4 * 2**20),
        )(*(pltpu.with_memory_space_constraint(x, pltpu.VMEM) for x in gathered))

    return jax.shard_map(
        local_block,
        mesh=mesh,
        in_specs=(P(("dp", "ro", "ri"), "co"), P(("ro", "ri"), "co")),
        out_specs=P(("dp", "ro", "ri", "co"), None),
        check_vma=False,
    )
```

```python
import functools

import jax
import jax.numpy as jnp
from jax import lax
from jax.experimental import pallas as pl
from jax.experimental.pallas import tpu as pltpu
from jax.sharding import PartitionSpec as P

MESH = pl.DeviceIdType.MESH
W = 256
ROWS = 256
OWN = ((0, 1024), (1024, 1024), (2048, 512), (3328, 768), (2560, 768))
VIA_Y = (
    (0, 1024, 0),
    (1024, 512, 1),
    (1536, 512, 1),
    (2048, 256, 2),
    (2304, 256, 2),
    (3328, 256, 3),
    (3584, 128, 3),
    (3712, 128, 3),
)
VIA_X = ((2560, 256, 4), (2816, 256, 4), (3072, 256, 4), (3840, 128, 4), (3968, 128, 4))
STRIPES = (
    (0, 0, 2560),
    (0, 3328, 768),
    (0, 2560, 768),
    (1, 0, 2304),
    (1, 2560, 256),
    (1, 2304, 256),
    (1, 2816, 512),
)
LAST = 3328


def _gather(a_ref, b_ref, abuf, bbuf, c_ref, x_send, y_send, p_send, x_recv, y_recv, p_recv, l_sem):
    ri, co, ro = lax.axis_index("ri"), lax.axis_index("co"), lax.axis_index("ro")
    to_x, to_y, to_p = {"co": 1 - co}, {"ri": 1 - ri}, {"ro": 1 - ro}
    depth, half = b_ref.shape
    rows, k_half = a_ref.shape[0] // 2, a_ref.shape[1]

    mine = pl.ds(pl.multiple_of((ro * 2 + ri) * depth, depth), depth)
    other = pl.ds(pl.multiple_of((ro * 2 + 1 - ri) * depth, depth), depth)
    a_cols = pl.ds(pl.multiple_of(co * k_half, k_half), k_half)

    def remote(src, dst, send, recv, to):
        return pltpu.make_async_remote_copy(
            src_ref=src, dst_ref=dst, send_sem=send, recv_sem=recv, device_id=to, device_id_type=MESH
        )

    def over_x(src, dst, i):
        return remote(src, dst, x_send, x_recv.at[i], to_x)

    def over_y(src, dst, i):
        return remote(src, dst, y_send, y_recv.at[i], to_y)

    def over_p(src, dst, i):
        return remote(src, dst, p_send, p_recv.at[i], to_p)

    n = len(OWN)
    cut = lambda h, k_rows, piece: bbuf.at[h, k_rows, pl.ds(piece[0], piece[1])]
    own = [cut(0, mine, OWN[0])] + [b_ref.at[:, pl.ds(*piece)] for piece in OWN[1:]]
    a_out = over_x(a_ref.at[pl.ds(pl.multiple_of((1 - co) * rows, rows), rows), :], abuf.at[:, a_cols], 0)
    a_loc = pltpu.make_async_copy(
        a_ref.at[pl.ds(pl.multiple_of(co * rows, rows), rows), :], abuf.at[:, a_cols], l_sem.at[0]
    )
    first = OWN[0][1]
    b_first = pltpu.make_async_copy(b_ref.at[:, pl.ds(0, first)], cut(0, mine, OWN[0]), l_sem.at[1])
    rest = pl.ds(first, half - first)
    b_rest = pltpu.make_async_copy(b_ref.at[:, rest], bbuf.at[0, mine, rest], l_sem.at[2])
    x_own = [over_x(own[i], cut(1, mine, OWN[i]), 1 + i) for i in range(n)]
    y_own = [over_y(own[i], cut(0, mine, OWN[i]), i) for i in range(n)]
    x_rel = [over_x(cut(0, other, p), cut(1, other, p), 1 + n + i) for i, p in enumerate(VIA_X)]
    y_rel = [over_y(cut(1, mine, p), cut(1, mine, p), n + i) for i, p in enumerate(VIA_Y)]
    p_own = over_p(b_ref, bbuf.at[0, mine, :], 0)
    p_y = [over_p(cut(0, other, p), cut(0, other, p), 1 + i) for i, p in enumerate(OWN)]
    p_x = [over_p(cut(1, mine, p), cut(1, mine, p), 1 + n + i) for i, p in enumerate(OWN)]
    p_dy = [over_p(cut(1, other, p), cut(1, other, p), 1 + 2 * n + i) for i, p in enumerate(VIA_Y)]
    p_dx = [over_p(cut(1, other, p), cut(1, other, p), 1 + 2 * n + len(VIA_Y) + i) for i, p in enumerate(VIA_X)]

    barrier = pltpu.get_barrier_semaphore()
    for to in (to_x, to_y, to_p):
        pl.semaphore_signal(barrier, inc=1, device_id=to, device_id_type=MESH)
    b_first.start()
    pl.semaphore_wait(barrier, 3)

    b_first.wait()
    x_own[0].start()
    y_own[0].start()
    a_out.start()
    for i in range(1, n):
        y_own[i].start()
        x_own[i].start()
    b_rest.start()
    a_loc.start()
    p_own.start()

    def from_y(i):
        y_own[i].wait_recv()
        p_y[i].start()
        for j, p in enumerate(VIA_X):
            if p[2] == i:
                x_rel[j].start()

    def from_x(i):
        x_own[i].wait_recv()
        p_x[i].start()
        for j, p in enumerate(VIA_Y):
            if p[2] == i:
                y_rel[j].start()

    def diagonal(i):
        y_rel[i].wait_recv()
        p_dy[i].start()

    def diagonal_x(i):
        x_rel[i].wait_recv()
        p_dx[i].start()

    def arrived(*copies):
        for copy in copies:
            copy.wait_recv()

    def before(step):
        if step == 0:
            from_y(0)
            from_x(0)
            from_y(1)
            from_y(2)
            from_y(3)
            a_loc.wait()
            b_rest.wait()
            arrived(p_own, a_out, *p_y[:4])
        elif step == 13:
            from_y(4)
            from_x(1)
            arrived(p_y[4])
        elif step == 16:
            diagonal(0)
            from_x(2)
            arrived(p_x[0], p_dy[0])
        elif step == 20:
            from_x(3)
            diagonal(1)
            from_x(4)
            diagonal(2)
            arrived(p_x[1], p_dy[1])
        elif step == 22:
            diagonal(3)
            diagonal_x(0)
            arrived(p_dy[2])
        elif step == 24:
            diagonal(4)
            diagonal_x(1)
            arrived(p_x[2], p_x[4], p_dy[3], p_dx[0])
        elif step == 26:
            diagonal(5)
            diagonal_x(2)
            arrived(p_dy[4], p_dx[1])
        elif step == 28:
            arrived(p_dx[2])

    steps = sum(size for _, _, size in STRIPES) // W

    @pl.loop(0, steps)
    def _(step):
        for at in (0, 13, 16, 20, 22, 24, 26, 28):
            pl.when(step == at)(functools.partial(before, at))
        h, col, seen = jnp.int32(0), jnp.int32(0), 0
        for side, start, size in STRIPES:
            here = step >= seen
            h = jnp.where(here, side, h)
            col = jnp.where(here, start + (step - seen) * W, col)
            seen += size // W
        cols = pl.ds(pl.multiple_of(col, W), W)
        c = jnp.dot(abuf[...], bbuf[h, :, cols], preferred_element_type=jnp.float32)
        c_ref[h, :, cols] = c.astype(c_ref.dtype)

    diagonal(6)
    diagonal_x(3)
    diagonal(7)
    diagonal_x(4)
    arrived(p_x[3], *p_dy[5:], *p_dx[3:])

    link = bbuf.at[0, pl.ds(0, 7 * k_half // 8), :]
    remote(link, link, x_send, x_recv.at[0], to_x).wait_send()
    remote(link, link, y_send, y_recv.at[0], to_y).wait_send()
    remote(bbuf.at[0], bbuf.at[0], p_send, p_recv.at[0], to_p).wait_send()


def _write(abuf, bbuf, c_ref, o_ref, last, sem):
    co = lax.axis_index("co")
    rows, half = c_ref.shape[1:]
    n = rows // ROWS
    near = pl.multiple_of(co * half, half)
    far = pl.multiple_of((1 - co) * half, half)

    tail = half - LAST

    def write(src, block, cols, i):
        return pltpu.make_async_copy(src, o_ref.at[block, cols], sem.at[i])

    whole = pl.ds(0, rows)
    near_out = write(c_ref.at[0], whole, pl.ds(near, half), n)
    far_out = write(c_ref.at[1, :, pl.ds(0, LAST)], whole, pl.ds(far, LAST), n + 1)

    def last_out(r):
        block = pl.ds(pl.multiple_of(r * ROWS, ROWS), ROWS)
        return write(last.at[block, :], block, pl.ds(pl.multiple_of(far + LAST, W), tail), r)

    near_out.start()
    far_out.start()

    @pl.loop(0, n)
    def _(r):
        block = pl.ds(pl.multiple_of(r * ROWS, ROWS), ROWS)
        c = jnp.dot(abuf[block, :], bbuf[1, :, LAST:], preferred_element_type=jnp.float32)
        last[block, :] = c.astype(last.dtype)
        last_out(r).start()

    near_out.wait()
    far_out.wait()

    @pl.loop(0, n)
    def _(r):
        last_out(r).wait()


def solution(mesh):
    def local_block(act_blk, weight_blk):
        rows, k = act_blk.shape[0] // 2, act_blk.shape[1] * 2
        half = weight_blk.shape[1]
        dma = pltpu.SemaphoreType.DMA
        vmem = pl.BlockSpec(memory_space=pltpu.VMEM)
        hbm = pl.BlockSpec(memory_space=pl.ANY)
        gathered = pl.pallas_call(
            _gather,
            out_shape=(
                pltpu.VMEM((rows, k), jnp.bfloat16),
                pltpu.VMEM((2, k, half), jnp.bfloat16),
                pltpu.VMEM((2, rows, half), jnp.bfloat16),
            ),
            in_specs=[hbm, hbm],
            out_specs=(vmem, vmem, vmem),
            scratch_shapes=[
                dma,
                dma,
                dma,
                dma((1 + len(OWN) + len(VIA_X),)),
                dma((len(OWN) + len(VIA_Y),)),
                dma((1 + 2 * len(OWN) + len(VIA_Y) + len(VIA_X),)),
                dma((3,)),
            ],
            compiler_params=pltpu.CompilerParams(
                collective_id=0, has_side_effects=True, vmem_limit_bytes=8 * 2**20
            ),
        )(
            pltpu.with_memory_space_constraint(act_blk, pltpu.HBM),
            pltpu.with_memory_space_constraint(weight_blk, pltpu.HBM),
        )
        return pl.pallas_call(
            _write,
            out_shape=jax.ShapeDtypeStruct((rows, 2 * half), jnp.bfloat16),
            in_specs=[vmem, vmem, vmem],
            out_specs=hbm,
            scratch_shapes=[pltpu.VMEM((rows, half - LAST), jnp.bfloat16), dma((rows // ROWS + 2,))],
            compiler_params=pltpu.CompilerParams(vmem_limit_bytes=8 * 2**20),
        )(*(pltpu.with_memory_space_constraint(x, pltpu.VMEM) for x in gathered))

    return jax.shard_map(
        local_block,
        mesh=mesh,
        in_specs=(P(("dp", "ro", "ri"), "co"), P(("ro", "ri"), "co")),
        out_specs=P(("dp", "ro", "ri", "co"), None),
        check_vma=False,
    )
```

```python
import functools

import jax
import jax.numpy as jnp
from jax import lax
from jax.experimental import pallas as pl
from jax.experimental.pallas import tpu as pltpu
from jax.sharding import PartitionSpec as P

MESH = pl.DeviceIdType.MESH
W = 256
ROWS = 256
OWN = ((0, 1024), (1024, 1024), (2048, 1280), (3328, 768))
VIA_Y = ((0, 1024, 0), (1024, 1024, 1), (2048, 512, 2), (3328, 256, 3), (3584, 128, 3), (3712, 128, 3))
VIA_X = ((2560, 512), (3072, 256), (3840, 128), (3968, 128))
LAST = 3328


def _gather(a_ref, b_ref, abuf, bbuf, c_ref, x_send, y_send, p_send, x_recv, y_recv, p_recv, l_sem):
    ri, co, ro = lax.axis_index("ri"), lax.axis_index("co"), lax.axis_index("ro")
    to_x, to_y, to_p = {"co": 1 - co}, {"ri": 1 - ri}, {"ro": 1 - ro}
    depth, half = b_ref.shape
    rows, k_half = a_ref.shape[0] // 2, a_ref.shape[1]

    mine = pl.ds(pl.multiple_of((ro * 2 + ri) * depth, depth), depth)
    other = pl.ds(pl.multiple_of((ro * 2 + 1 - ri) * depth, depth), depth)
    a_cols = pl.ds(pl.multiple_of(co * k_half, k_half), k_half)

    def remote(src, dst, send, recv, to):
        return pltpu.make_async_remote_copy(
            src_ref=src, dst_ref=dst, send_sem=send, recv_sem=recv, device_id=to, device_id_type=MESH
        )

    def over_x(src, dst, i):
        return remote(src, dst, x_send, x_recv.at[i], to_x)

    def over_y(src, dst, i):
        return remote(src, dst, y_send, y_recv.at[i], to_y)

    def over_p(src, dst, i):
        return remote(src, dst, p_send, p_recv.at[i], to_p)

    cut = lambda h, k_rows, piece: bbuf.at[h, k_rows, pl.ds(piece[0], piece[1])]
    a_out = over_x(a_ref.at[pl.ds(pl.multiple_of((1 - co) * rows, rows), rows), :], abuf.at[:, a_cols], 0)
    a_loc = pltpu.make_async_copy(
        a_ref.at[pl.ds(pl.multiple_of(co * rows, rows), rows), :], abuf.at[:, a_cols], l_sem.at[0]
    )
    b_loc = pltpu.make_async_copy(b_ref, bbuf.at[0, mine, :], l_sem.at[1])
    n = len(OWN)
    x_own = [over_x(b_ref.at[:, pl.ds(*p)], cut(1, mine, p), 1 + i) for i, p in enumerate(OWN)]
    x_rel = [over_x(cut(0, other, p), cut(1, other, p), 1 + n + i) for i, p in enumerate(VIA_X)]
    y_own = over_y(b_ref, bbuf.at[0, mine, :], 0)
    y_rel = [over_y(cut(1, mine, p), cut(1, mine, p), 1 + i) for i, p in enumerate(VIA_Y)]

    p_own = over_p(b_ref, bbuf.at[0, mine, :], 0)
    p_y = over_p(bbuf.at[0, other, :], bbuf.at[0, other, :], 0)
    p_x = [over_p(cut(1, mine, p), cut(1, mine, p), i) for p, i in zip(OWN, (2, 3, 4, 1))]
    p_dy = [over_p(cut(1, other, p), cut(1, other, p), i) for p, i in zip(VIA_Y, (5, 6, 7, 1, 1, 1))]
    p_dx = [over_p(cut(1, other, p), cut(1, other, p), i) for p, i in zip(VIA_X, (8, 9, 1, 1))]
    near_half = over_p(bbuf.at[0, pl.ds(0, 2 * depth), :], bbuf.at[0, pl.ds(0, 2 * depth), :], 0)
    late = pl.ds(0, 2 * (half - LAST) * depth // half)
    late_parts = over_p(bbuf.at[0, late, :], bbuf.at[0, late, :], 1)

    barrier = pltpu.get_barrier_semaphore()
    for to in (to_x, to_y, to_p):
        pl.semaphore_signal(barrier, inc=1, device_id=to, device_id_type=MESH)
    pl.semaphore_wait(barrier, 3)

    x_own[0].start()
    y_own.start()
    a_out.start()
    for copy in x_own[1:]:
        copy.start()
    b_loc.start()
    a_loc.start()
    p_own.start()

    def from_y():
        y_own.wait_recv()
        p_y.start()
        for copy in x_rel:
            copy.start()

    def from_x(i):
        x_own[i].wait_recv()
        p_x[i].start()
        for j, p in enumerate(VIA_Y):
            if p[2] == i:
                y_rel[j].start()

    def diagonal(i):
        y_rel[i].wait_recv()
        p_dy[i].start()

    def diagonal_x(i):
        x_rel[i].wait_recv()
        p_dx[i].start()

    def arrived(*copies):
        for copy in copies:
            copy.wait_recv()

    def before(step):
        if step == 0:
            from_x(0)
            from_y()
            from_x(1)
            a_loc.wait()
            b_loc.wait()
            arrived(a_out, near_half)
        elif step == 12:
            diagonal(0)
        elif step == 16:
            from_x(2)
            arrived(p_x[0], p_dy[0])
        elif step == 20:
            from_x(3)
            diagonal(1)
            arrived(p_x[1], p_dy[1])
        elif step == 24:
            diagonal(2)
            diagonal_x(0)
            arrived(p_x[2], p_dy[2], p_dx[0])
        elif step == 27:
            diagonal(3)
            diagonal_x(1)
        elif step == 28:
            arrived(p_dx[1])

    @pl.loop(0, (half + LAST) // W)
    def _(step):
        for at in (0, 12, 16, 20, 24, 27, 28):
            pl.when(step == at)(functools.partial(before, at))
        h = step // (half // W)
        cols = pl.ds(pl.multiple_of(step * W - h * half, W), W)
        c = jnp.dot(abuf[...], bbuf[h, :, cols], preferred_element_type=jnp.float32)
        c_ref[h, :, cols] = c.astype(c_ref.dtype)

    for i in (4, 5):
        diagonal(i)
        diagonal_x(i - 2)
    arrived(late_parts)

    link = bbuf.at[0, pl.ds(0, 7 * k_half // 8), :]
    remote(link, link, x_send, x_recv.at[0], to_x).wait_send()
    remote(link, link, y_send, y_recv.at[0], to_y).wait_send()
    remote(bbuf.at[0], bbuf.at[0], p_send, p_recv.at[0], to_p).wait_send()


def _write(abuf, bbuf, c_ref, o_ref, last, sem):
    co = lax.axis_index("co")
    rows, half = c_ref.shape[1:]
    n = rows // ROWS
    near = pl.multiple_of(co * half, half)
    far = pl.multiple_of((1 - co) * half, half)

    tail = half - LAST

    def write(src, block, cols, i):
        return pltpu.make_async_copy(src, o_ref.at[block, cols], sem.at[i])

    whole = pl.ds(0, rows)
    near_out = write(c_ref.at[0], whole, pl.ds(near, half), n)
    far_out = write(c_ref.at[1, :, pl.ds(0, LAST)], whole, pl.ds(far, LAST), n + 1)

    def last_out(r):
        block = pl.ds(pl.multiple_of(r * ROWS, ROWS), ROWS)
        return write(last.at[block, :], block, pl.ds(pl.multiple_of(far + LAST, W), tail), r)

    near_out.start()
    far_out.start()

    @pl.loop(0, n)
    def _(r):
        block = pl.ds(pl.multiple_of(r * ROWS, ROWS), ROWS)
        c = jnp.dot(abuf[block, :], bbuf[1, :, LAST:], preferred_element_type=jnp.float32)
        last[block, :] = c.astype(last.dtype)
        last_out(r).start()

    near_out.wait()
    far_out.wait()

    @pl.loop(0, n)
    def _(r):
        last_out(r).wait()


def solution(mesh):
    def local_block(act_blk, weight_blk):
        rows, k = act_blk.shape[0] // 2, act_blk.shape[1] * 2
        half = weight_blk.shape[1]
        dma = pltpu.SemaphoreType.DMA
        vmem = pl.BlockSpec(memory_space=pltpu.VMEM)
        hbm = pl.BlockSpec(memory_space=pl.ANY)
        gathered = pl.pallas_call(
            _gather,
            out_shape=(
                pltpu.VMEM((rows, k), jnp.bfloat16),
                pltpu.VMEM((2, k, half), jnp.bfloat16),
                pltpu.VMEM((2, rows, half), jnp.bfloat16),
            ),
            in_specs=[hbm, hbm],
            out_specs=(vmem, vmem, vmem),
            scratch_shapes=[
                dma,
                dma,
                dma,
                dma((1 + len(OWN) + len(VIA_X),)),
                dma((1 + len(VIA_Y),)),
                dma((10,)),
                dma((2,)),
            ],
            compiler_params=pltpu.CompilerParams(
                collective_id=0, has_side_effects=True, vmem_limit_bytes=8 * 2**20
            ),
        )(
            pltpu.with_memory_space_constraint(act_blk, pltpu.HBM),
            pltpu.with_memory_space_constraint(weight_blk, pltpu.HBM),
        )
        return pl.pallas_call(
            _write,
            out_shape=jax.ShapeDtypeStruct((rows, 2 * half), jnp.bfloat16),
            in_specs=[vmem, vmem, vmem],
            out_specs=hbm,
            scratch_shapes=[pltpu.VMEM((rows, half - LAST), jnp.bfloat16), dma((rows // ROWS + 2,))],
            compiler_params=pltpu.CompilerParams(vmem_limit_bytes=8 * 2**20),
        )(*(pltpu.with_memory_space_constraint(x, pltpu.VMEM) for x in gathered))

    return jax.shard_map(
        local_block,
        mesh=mesh,
        in_specs=(P(("dp", "ro", "ri"), "co"), P(("ro", "ri"), "co")),
        out_specs=P(("dp", "ro", "ri", "co"), None),
        check_vma=False,
    )
```

```python
import functools

import jax
import jax.numpy as jnp
from jax import lax
from jax.experimental import pallas as pl
from jax.experimental.pallas import tpu as pltpu
from jax.sharding import PartitionSpec as P

MESH = pl.DeviceIdType.MESH
W = 256
ROWS = 256
OWN = ((0, 1024), (1024, 1024), (2048, 1280), (3328, 768))
VIA_Y = (
    ((0, 1024),),
    ((1024, 1024),),
    ((2048, 512),),
    ((3328, 256), (3584, 128), (3712, 128, 0, 384), (3712, 128, 384, 512)),
)
VIA_X = ((2560, 512), (3072, 256), (3840, 128), (3968, 128, 0, 384), (3968, 128, 384, 512))
LAST = 3328


def _gather(a_ref, b_ref, abuf, bbuf, c_ref, x_send, y_send, p_send, x_recv, y_recv, p_recv, l_sem):
    ri, co, ro = lax.axis_index("ri"), lax.axis_index("co"), lax.axis_index("ro")
    to_x, to_y, to_p = {"co": 1 - co}, {"ri": 1 - ri}, {"ro": 1 - ro}
    depth, half = b_ref.shape
    rows, k_half = a_ref.shape[0] // 2, a_ref.shape[1]

    mine = (ro * 2 + ri) * depth
    other = (ro * 2 + 1 - ri) * depth
    a_cols = pl.ds(pl.multiple_of(co * k_half, k_half), k_half)

    def remote(src, dst, send, recv, to):
        return pltpu.make_async_remote_copy(
            src_ref=src, dst_ref=dst, send_sem=send, recv_sem=recv, device_id=to, device_id_type=MESH
        )

    def over_x(src, dst, i):
        return remote(src, dst, x_send, x_recv.at[i], to_x)

    def over_y(src, dst, i):
        return remote(src, dst, y_send, y_recv.at[i], to_y)

    def over_p(src, dst, i):
        return remote(src, dst, p_send, p_recv.at[i], to_p)


    def cut(h, block, piece):
        start, size, r0, r1 = (*piece, 0, depth)[:4] if len(piece) == 2 else piece
        return bbuf.at[h, pl.ds(pl.multiple_of(block + r0, 128), r1 - r0), pl.ds(start, size)]
    a_out = over_x(a_ref.at[pl.ds(pl.multiple_of((1 - co) * rows, rows), rows), :], abuf.at[:, a_cols], 0)
    a_loc = pltpu.make_async_copy(
        a_ref.at[pl.ds(pl.multiple_of(co * rows, rows), rows), :], abuf.at[:, a_cols], l_sem.at[0]
    )
    b_loc = pltpu.make_async_copy(b_ref, cut(0, mine, (0, half)), l_sem.at[1])
    n = len(OWN)
    x_own = [over_x(b_ref.at[:, pl.ds(*p)], cut(1, mine, p), 1 + i) for i, p in enumerate(OWN)]
    x_rel = [over_x(cut(0, other, p), cut(1, other, p), 1 + n + i) for i, p in enumerate(VIA_X)]
    y_own = over_y(b_ref, cut(0, mine, (0, half)), 0)
    via_y = sum(VIA_Y, ())
    y_rel = [over_y(cut(1, mine, p), cut(1, mine, p), 1 + i) for i, p in enumerate(via_y)]

    p_own = over_p(b_ref, cut(0, mine, (0, half)), 0)
    p_y = over_p(cut(0, other, (0, half)), cut(0, other, (0, half)), 0)
    p_x = [over_p(cut(1, mine, p), cut(1, mine, p), i) for p, i in zip(OWN, (2, 3, 4, 1))]
    p_dy = [over_p(cut(1, other, p), cut(1, other, p), i) for p, i in zip(via_y, (5, 6, 7, 1, 1, 1, 1))]
    p_dx = [over_p(cut(1, other, p), cut(1, other, p), i) for p, i in zip(VIA_X, (8, 9, 1, 1, 1))]
    near_half = over_p(bbuf.at[0, pl.ds(0, 2 * depth), :], bbuf.at[0, pl.ds(0, 2 * depth), :], 0)
    late = pl.ds(0, 2 * (half - LAST) * depth // half)
    late_parts = over_p(bbuf.at[0, late, :], bbuf.at[0, late, :], 1)

    barrier = pltpu.get_barrier_semaphore()
    for to in (to_x, to_y, to_p):
        pl.semaphore_signal(barrier, inc=1, device_id=to, device_id_type=MESH)
    pl.semaphore_wait(barrier, 3)

    x_own[0].start()
    y_own.start()
    a_out.start()
    for copy in x_own[1:]:
        copy.start()
    b_loc.start()
    a_loc.start()
    p_own.start()

    def from_y():
        y_own.wait_recv()
        p_y.start()
        for copy in x_rel:
            copy.start()

    def from_x(i):
        x_own[i].wait_recv()
        p_x[i].start()
        first = sum(len(parts) for parts in VIA_Y[:i])
        for copy in y_rel[first : first + len(VIA_Y[i])]:
            copy.start()

    def diagonal(i):
        y_rel[i].wait_recv()
        p_dy[i].start()

    def diagonal_x(i):
        x_rel[i].wait_recv()
        p_dx[i].start()

    def arrived(*copies):
        for copy in copies:
            copy.wait_recv()

    def before(step):
        if step == 0:
            from_x(0)
            from_y()
            from_x(1)
            a_loc.wait()
            b_loc.wait()
            arrived(a_out, near_half)
        elif step == 12:
            diagonal(0)
        elif step == 16:
            from_x(2)
            arrived(p_x[0], p_dy[0])
        elif step == 20:
            from_x(3)
            diagonal(1)
            arrived(p_x[1], p_dy[1])
        elif step == 24:
            diagonal(2)
            diagonal_x(0)
            arrived(p_x[2], p_dy[2], p_dx[0])
        elif step == 27:
            diagonal(3)
            diagonal_x(1)
        elif step == 28:
            arrived(p_dx[1])

    @pl.loop(0, (half + LAST) // W)
    def _(step):
        for at in (0, 12, 16, 20, 24, 27, 28):
            pl.when(step == at)(functools.partial(before, at))
        h = step // (half // W)
        cols = pl.ds(pl.multiple_of(step * W - h * half, W), W)
        c = jnp.dot(abuf[...], bbuf[h, :, cols], preferred_element_type=jnp.float32)
        c_ref[h, :, cols] = c.astype(c_ref.dtype)

    for i in (4, 5, 6):
        diagonal(i)
        diagonal_x(i - 2)
    arrived(late_parts)

    link = bbuf.at[0, pl.ds(0, 7 * k_half // 8), :]
    remote(link, link, x_send, x_recv.at[0], to_x).wait_send()
    remote(link, link, y_send, y_recv.at[0], to_y).wait_send()
    remote(bbuf.at[0], bbuf.at[0], p_send, p_recv.at[0], to_p).wait_send()


def _write(abuf, bbuf, c_ref, o_ref, last, sem):
    co = lax.axis_index("co")
    rows, half = c_ref.shape[1:]
    n = rows // ROWS
    near = pl.multiple_of(co * half, half)
    far = pl.multiple_of((1 - co) * half, half)

    tail = half - LAST

    def write(src, block, cols, i):
        return pltpu.make_async_copy(src, o_ref.at[block, cols], sem.at[i])

    ready = []
    for i in range(2):
        block = pl.ds(i * rows // 2, rows // 2)
        ready.append(write(c_ref.at[0, block, :], block, pl.ds(near, half), n + 2 * i))
        ready.append(write(c_ref.at[1, block, pl.ds(0, LAST)], block, pl.ds(far, LAST), n + 2 * i + 1))

    def last_out(r):
        block = pl.ds(pl.multiple_of(r * ROWS, ROWS), ROWS)
        return write(last.at[block, :], block, pl.ds(pl.multiple_of(far + LAST, W), tail), r)

    for copy in ready:
        copy.start()

    @pl.loop(0, n)
    def _(r):
        block = pl.ds(pl.multiple_of(r * ROWS, ROWS), ROWS)
        c = jnp.dot(abuf[block, :], bbuf[1, :, LAST:], preferred_element_type=jnp.float32)
        last[block, :] = c.astype(last.dtype)
        last_out(r).start()

    for copy in ready:
        copy.wait()

    @pl.loop(0, n)
    def _(r):
        last_out(r).wait()


def solution(mesh):
    def local_block(act_blk, weight_blk):
        rows, k = act_blk.shape[0] // 2, act_blk.shape[1] * 2
        half = weight_blk.shape[1]
        dma = pltpu.SemaphoreType.DMA
        vmem = pl.BlockSpec(memory_space=pltpu.VMEM)
        hbm = pl.BlockSpec(memory_space=pl.ANY)
        gathered = pl.pallas_call(
            _gather,
            out_shape=(
                pltpu.VMEM((rows, k), jnp.bfloat16),
                pltpu.VMEM((2, k, half), jnp.bfloat16),
                pltpu.VMEM((2, rows, half), jnp.bfloat16),
            ),
            in_specs=[hbm, hbm],
            out_specs=(vmem, vmem, vmem),
            scratch_shapes=[
                dma,
                dma,
                dma,
                dma((1 + len(OWN) + len(VIA_X),)),
                dma((1 + len(sum(VIA_Y, ())),)),
                dma((10,)),
                dma((2,)),
            ],
            compiler_params=pltpu.CompilerParams(
                collective_id=0, has_side_effects=True, vmem_limit_bytes=8 * 2**20
            ),
        )(
            pltpu.with_memory_space_constraint(act_blk, pltpu.HBM),
            pltpu.with_memory_space_constraint(weight_blk, pltpu.HBM),
        )
        return pl.pallas_call(
            _write,
            out_shape=jax.ShapeDtypeStruct((rows, 2 * half), jnp.bfloat16),
            in_specs=[vmem, vmem, vmem],
            out_specs=hbm,
            scratch_shapes=[pltpu.VMEM((rows, half - LAST), jnp.bfloat16), dma((rows // ROWS + 4,))],
            compiler_params=pltpu.CompilerParams(vmem_limit_bytes=8 * 2**20),
        )(*(pltpu.with_memory_space_constraint(x, pltpu.VMEM) for x in gathered))

    return jax.shard_map(
        local_block,
        mesh=mesh,
        in_specs=(P(("dp", "ro", "ri"), "co"), P(("ro", "ri"), "co")),
        out_specs=P(("dp", "ro", "ri", "co"), None),
        check_vma=False,
    )
```

```python
import functools

import jax
import jax.numpy as jnp
from jax import lax
from jax.experimental import pallas as pl
from jax.experimental.pallas import tpu as pltpu
from jax.sharding import PartitionSpec as P

MESH = pl.DeviceIdType.MESH
W = 256
ROWS = 256
OWN = ((0, 2048), (2048, 1280), (3328, 768))
VIA_Y = (
    ((0, 1024), (1024, 1024)),
    ((2048, 512),),
    ((3328, 256), (3584, 128), (3712, 128, 0, 384), (3712, 128, 384, 512)),
)
VIA_X = ((2560, 512), (3072, 256), (3840, 128), (3968, 128, 0, 384), (3968, 128, 384, 512))
LAST = 3328


def _gather(a_ref, b_ref, abuf, bbuf, c_ref, send, x_recv, y_recv, p_recv, l_sem):
    ri, co, ro = lax.axis_index("ri"), lax.axis_index("co"), lax.axis_index("ro")
    to_x, to_y, to_p = {"co": 1 - co}, {"ri": 1 - ri}, {"ro": 1 - ro}
    depth, half = b_ref.shape
    rows, k_half = a_ref.shape[0] // 2, a_ref.shape[1]

    mine = (ro * 2 + ri) * depth
    other = (ro * 2 + 1 - ri) * depth
    a_cols = pl.ds(pl.multiple_of(co * k_half, k_half), k_half)

    def remote(src, dst, send, recv, to):
        return pltpu.make_async_remote_copy(
            src_ref=src, dst_ref=dst, send_sem=send, recv_sem=recv, device_id=to, device_id_type=MESH
        )

    def over_x(src, dst, i):
        return remote(src, dst, send, x_recv.at[i], to_x)

    def over_y(src, dst, i):
        return remote(src, dst, send, y_recv.at[i], to_y)

    def over_p(src, dst, i):
        return remote(src, dst, send, p_recv.at[i], to_p)


    def cut(h, block, piece):
        start, size, r0, r1 = (*piece, 0, depth)[:4] if len(piece) == 2 else piece
        return bbuf.at[h, pl.ds(pl.multiple_of(block + r0, 128), r1 - r0), pl.ds(start, size)]
    a_out = over_x(a_ref.at[pl.ds(pl.multiple_of((1 - co) * rows, rows), rows), :], abuf.at[:, a_cols], 0)
    a_loc = pltpu.make_async_copy(
        a_ref.at[pl.ds(pl.multiple_of(co * rows, rows), rows), :], abuf.at[:, a_cols], l_sem
    )
    b_loc = pltpu.make_async_copy(b_ref, cut(0, mine, (0, half)), l_sem)
    loaded = bbuf.at[0, pl.ds(0, 3 * k_half // 4), :]
    n = len(OWN)
    x_own = [over_x(b_ref.at[:, pl.ds(*p)], cut(1, mine, p), 1 + i) for i, p in enumerate(OWN)]
    x_rel = [over_x(cut(0, other, p), cut(1, other, p), 1 + n + i) for i, p in enumerate(VIA_X)]
    y_own = over_y(b_ref, cut(0, mine, (0, half)), 0)
    via_y = sum(VIA_Y, ())
    y_rel = [over_y(cut(1, mine, p), cut(1, mine, p), 1 + i) for i, p in enumerate(via_y)]

    p_own = over_p(b_ref, cut(0, mine, (0, half)), 0)
    p_y = over_p(cut(0, other, (0, half)), cut(0, other, (0, half)), 0)
    p_x = [over_p(cut(1, mine, p), cut(1, mine, p), i) for p, i in zip(OWN, (2, 4, 1))]
    p_dy = [over_p(cut(1, other, p), cut(1, other, p), i) for p, i in zip(via_y, (2, 3, 4, 1, 1, 1, 1))]
    p_dx = [over_p(cut(1, other, p), cut(1, other, p), i) for p, i in zip(VIA_X, (4, 5, 1, 1, 1))]
    near_half = over_p(bbuf.at[0, pl.ds(0, 2 * depth), :], bbuf.at[0, pl.ds(0, 2 * depth), :], 0)

    def both(cols, i):
        rows_in_all = pl.ds(0, cols * depth // half)
        return over_p(bbuf.at[0, rows_in_all, :], bbuf.at[0, rows_in_all, :], i)

    late_parts = both(2 * (half - LAST), 1)
    first_parts = both(2048 + 1024, 2)
    next_parts = both(1280 + 512 + 512, 4)

    barrier = pltpu.get_barrier_semaphore()
    for to in (to_x, to_y, to_p):
        pl.semaphore_signal(barrier, inc=1, device_id=to, device_id_type=MESH)
    pl.semaphore_wait(barrier, 3)

    x_own[0].start()
    y_own.start()
    a_out.start()
    for copy in x_own[1:]:
        copy.start()
    b_loc.start()
    a_loc.start()
    p_own.start()

    def from_y():
        y_own.wait_recv()
        p_y.start()
        for copy in x_rel:
            copy.start()

    def from_x(i):
        x_own[i].wait_recv()
        p_x[i].start()
        first = sum(len(parts) for parts in VIA_Y[:i])
        for copy in y_rel[first : first + len(VIA_Y[i])]:
            copy.start()

    def diagonal(i):
        y_rel[i].wait_recv()
        p_dy[i].start()

    def diagonal_x(i):
        x_rel[i].wait_recv()
        p_dx[i].start()

    def arrived(*copies):
        for copy in copies:
            copy.wait_recv()

    def before(step):
        if step == 0:
            from_x(0)
            from_y()
            pltpu.make_async_copy(loaded, loaded, l_sem).wait()
            arrived(a_out, near_half)
        elif step == 12:
            diagonal(0)
        elif step == 16:
            from_x(1)
            arrived(first_parts)
        elif step == 20:
            from_x(2)
            diagonal(1)
            arrived(p_dy[1])
        elif step == 24:
            diagonal(2)
            diagonal_x(0)
            arrived(next_parts)
        elif step == 27:
            diagonal(3)
            diagonal_x(1)
        elif step == 28:
            arrived(p_dx[1])

    @pl.loop(0, (half + LAST) // W)
    def _(step):
        for at in (0, 12, 16, 20, 24, 27, 28):
            pl.when(step == at)(functools.partial(before, at))
        h = step // (half // W)
        cols = pl.ds(pl.multiple_of(step * W - h * half, W), W)
        c = jnp.dot(abuf[...], bbuf[h, :, cols], preferred_element_type=jnp.float32)
        c_ref[h, :, cols] = c.astype(c_ref.dtype)

    for i in (4, 5, 6):
        diagonal(i)
        diagonal_x(i - 2)
    arrived(late_parts)

    sent = bbuf.at[:, pl.ds(0, 15 * k_half // 8), :]
    remote(sent, sent, send, p_recv.at[0], to_p).wait_send()


def _write(abuf, bbuf, c_ref, o_ref, last, sem):
    co = lax.axis_index("co")
    rows, half = c_ref.shape[1:]
    n = rows // ROWS
    near = pl.multiple_of(co * half, half)
    far = pl.multiple_of((1 - co) * half, half)

    tail = half - LAST

    def write(src, block, cols):
        return pltpu.make_async_copy(src, o_ref.at[block, cols], sem)

    ready = []
    for i in range(2):
        block = pl.ds(i * rows // 2, rows // 2)
        ready.append(write(c_ref.at[0, block, :], block, pl.ds(near, half)))
        ready.append(write(c_ref.at[1, block, pl.ds(0, LAST)], block, pl.ds(far, LAST)))

    def last_out(r):
        block = pl.ds(pl.multiple_of(r * ROWS, ROWS), ROWS)
        return write(last.at[block, :], block, pl.ds(pl.multiple_of(far + LAST, W), tail))

    for copy in ready:
        copy.start()

    @pl.loop(0, n)
    def _(r):
        block = pl.ds(pl.multiple_of(r * ROWS, ROWS), ROWS)
        c = jnp.dot(abuf[block, :], bbuf[1, :, LAST:], preferred_element_type=jnp.float32)
        last[block, :] = c.astype(last.dtype)
        last_out(r).start()

    pltpu.make_async_copy(c_ref, c_ref, sem).wait()


def solution(mesh):
    def local_block(act_blk, weight_blk):
        rows, k = act_blk.shape[0] // 2, act_blk.shape[1] * 2
        half = weight_blk.shape[1]
        dma = pltpu.SemaphoreType.DMA
        vmem = pl.BlockSpec(memory_space=pltpu.VMEM)
        hbm = pl.BlockSpec(memory_space=pl.ANY)
        gathered = pl.pallas_call(
            _gather,
            out_shape=(
                pltpu.VMEM((rows, k), jnp.bfloat16),
                pltpu.VMEM((2, k, half), jnp.bfloat16),
                pltpu.VMEM((2, rows, half), jnp.bfloat16),
            ),
            in_specs=[hbm, hbm],
            out_specs=(vmem, vmem, vmem),
            scratch_shapes=[
                dma,
                dma((1 + len(OWN) + len(VIA_X),)),
                dma((1 + len(sum(VIA_Y, ())),)),
                dma((6,)),
                dma,
            ],
            compiler_params=pltpu.CompilerParams(
                collective_id=0, has_side_effects=True, vmem_limit_bytes=8 * 2**20
            ),
        )(
            pltpu.with_memory_space_constraint(act_blk, pltpu.HBM),
            pltpu.with_memory_space_constraint(weight_blk, pltpu.HBM),
        )
        return pl.pallas_call(
            _write,
            out_shape=jax.ShapeDtypeStruct((rows, 2 * half), jnp.bfloat16),
            in_specs=[vmem, vmem, vmem],
            out_specs=hbm,
            scratch_shapes=[pltpu.VMEM((rows, half - LAST), jnp.bfloat16), dma],
            compiler_params=pltpu.CompilerParams(vmem_limit_bytes=8 * 2**20),
        )(*(pltpu.with_memory_space_constraint(x, pltpu.VMEM) for x in gathered))

    return jax.shard_map(
        local_block,
        mesh=mesh,
        in_specs=(P(("dp", "ro", "ri"), "co"), P(("ro", "ri"), "co")),
        out_specs=P(("dp", "ro", "ri", "co"), None),
        check_vma=False,
    )
```

```python
import functools

import jax
import jax.numpy as jnp
from jax import lax
from jax.experimental import pallas as pl
from jax.experimental.pallas import tpu as pltpu
from jax.sharding import PartitionSpec as P

MESH = pl.DeviceIdType.MESH
W = 256
ROWS = 256
OWN = ((0, 2048), (2048, 1280), (3328, 768))
VIA_Y = (
    ((0, 1024), (1024, 1024)),
    ((2048, 512),),
    ((3328, 256), (3584, 128), (3712, 128, 0, 256), (3712, 128, 256, 512)),
)
VIA_X = ((2560, 512), (3072, 256), (3840, 128), (3968, 128, 0, 256), (3968, 128, 256, 512))
LAST = 3328


def _gather(a_ref, b_ref, abuf, bbuf, c_ref, send, x_recv, y_recv, p_recv, l_sem):
    ri, co, ro = lax.axis_index("ri"), lax.axis_index("co"), lax.axis_index("ro")
    to_x, to_y, to_p = {"co": 1 - co}, {"ri": 1 - ri}, {"ro": 1 - ro}
    depth, half = b_ref.shape
    rows, k_half = a_ref.shape[0] // 2, a_ref.shape[1]

    mine = (ro * 2 + ri) * depth
    other = (ro * 2 + 1 - ri) * depth
    a_cols = pl.ds(pl.multiple_of(co * k_half, k_half), k_half)

    def remote(src, dst, send, recv, to):
        return pltpu.make_async_remote_copy(
            src_ref=src, dst_ref=dst, send_sem=send, recv_sem=recv, device_id=to, device_id_type=MESH
        )

    def over_x(src, dst, i):
        return remote(src, dst, send, x_recv.at[i], to_x)

    def over_y(src, dst, i):
        return remote(src, dst, send, y_recv.at[i], to_y)

    def over_p(src, dst, i):
        return remote(src, dst, send, p_recv.at[i], to_p)


    def cut(h, block, piece):
        start, size, r0, r1 = (*piece, 0, depth)[:4] if len(piece) == 2 else piece
        return bbuf.at[h, pl.ds(pl.multiple_of(block + r0, 64), r1 - r0), pl.ds(start, size)]
    a_out = over_x(a_ref.at[pl.ds(pl.multiple_of((1 - co) * rows, rows), rows), :], abuf.at[:, a_cols], 0)
    a_loc = pltpu.make_async_copy(
        a_ref.at[pl.ds(pl.multiple_of(co * rows, rows), rows), :], abuf.at[:, a_cols], l_sem
    )
    b_loc = pltpu.make_async_copy(b_ref, cut(0, mine, (0, half)), l_sem)
    loaded = bbuf.at[0, pl.ds(0, 3 * k_half // 4), :]
    n = len(OWN)
    x_own = [over_x(b_ref.at[:, pl.ds(*p)], cut(1, mine, p), 1 + i) for i, p in enumerate(OWN)]
    x_rel = [over_x(cut(0, other, p), cut(1, other, p), 1 + n + i) for i, p in enumerate(VIA_X)]
    direct_x = remote(
        cut(0, other, VIA_X[-1]),
        cut(1, other, VIA_X[-1]),
        send,
        x_recv.at[1 + n + len(VIA_X)],
        {"co": 1 - co, "ro": 1 - ro},
    )
    via_y = sum(VIA_Y, ())
    direct_y = remote(
        cut(1, mine, via_y[-1]),
        cut(1, mine, via_y[-1]),
        send,
        y_recv.at[1 + len(via_y)],
        {"ri": 1 - ri, "ro": 1 - ro},
    )
    y_own = over_y(b_ref, cut(0, mine, (0, half)), 0)
    y_rel = [over_y(cut(1, mine, p), cut(1, mine, p), 1 + i) for i, p in enumerate(via_y)]

    p_own = over_p(b_ref, cut(0, mine, (0, half)), 0)
    p_y = over_p(cut(0, other, (0, half)), cut(0, other, (0, half)), 0)
    p_x = [over_p(cut(1, mine, p), cut(1, mine, p), i) for p, i in zip(OWN, (2, 4, 1))]
    p_dy = [over_p(cut(1, other, p), cut(1, other, p), i) for p, i in zip(via_y, (2, 3, 4, 1, 1, 1, 1))]
    p_dx = [over_p(cut(1, other, p), cut(1, other, p), i) for p, i in zip(VIA_X, (4, 5, 1, 1, 1))]
    near_half = over_p(bbuf.at[0, pl.ds(0, 2 * depth), :], bbuf.at[0, pl.ds(0, 2 * depth), :], 0)

    def both(cols, i):
        rows_in_all = pl.ds(0, cols * depth // half)
        return over_p(bbuf.at[0, rows_in_all, :], bbuf.at[0, rows_in_all, :], i)

    late_parts = both(2 * (half - LAST), 1)
    less = bbuf.at[0, pl.ds(0, 176), pl.ds(0, 4096)]
    late_parts_less = over_p(less, less, 1)
    first_parts = both(2048 + 1024, 2)
    next_parts = both(1280 + 512 + 512, 4)

    barrier = pltpu.get_barrier_semaphore()
    for to in (to_x, to_y, to_p):
        pl.semaphore_signal(barrier, inc=1, device_id=to, device_id_type=MESH)
    pl.semaphore_wait(barrier, 3)

    x_own[0].start()
    y_own.start()
    a_out.start()
    for copy in x_own[1:]:
        copy.start()
    b_loc.start()
    a_loc.start()
    p_own.start()

    def from_y():
        y_own.wait_recv()
        p_y.start()
        for copy in x_rel:
            copy.start()
        pl.when(ro == 0)(direct_x.start)

    def from_x(i):
        x_own[i].wait_recv()
        p_x[i].start()
        first = sum(len(parts) for parts in VIA_Y[:i])
        for copy in y_rel[first : first + len(VIA_Y[i])]:
            copy.start()
        if i == len(VIA_Y) - 1:
            pl.when(ro == 0)(direct_y.start)

    def diagonal(i):
        y_rel[i].wait_recv()
        p_dy[i].start()

    def diagonal_x(i):
        x_rel[i].wait_recv()
        p_dx[i].start()

    def arrived(*copies):
        for copy in copies:
            copy.wait_recv()

    def before(step):
        if step == 0:
            from_x(0)
            from_y()
            pltpu.make_async_copy(loaded, loaded, l_sem).wait()
            arrived(a_out, near_half)
        elif step == 12:
            diagonal(0)
        elif step == 16:
            from_x(1)
            arrived(first_parts)
        elif step == 20:
            from_x(2)
            diagonal(1)
            arrived(p_dy[1])
        elif step == 24:
            diagonal(2)
            diagonal_x(0)
            arrived(next_parts)
        elif step == 27:
            diagonal(3)
            diagonal_x(1)
        elif step == 28:
            arrived(p_dx[1])

    @pl.loop(0, (half + LAST) // W)
    def _(step):
        for at in (0, 12, 16, 20, 24, 27, 28):
            pl.when(step == at)(functools.partial(before, at))
        h = step // (half // W)
        cols = pl.ds(pl.multiple_of(step * W - h * half, W), W)
        c = jnp.dot(abuf[...], bbuf[h, :, cols], preferred_element_type=jnp.float32)
        c_ref[h, :, cols] = c.astype(c_ref.dtype)

    for i in (4, 5):
        diagonal(i)
        diagonal_x(i - 2)

    @pl.when(ro == 0)
    def _():
        arrived(y_rel[6], x_rel[4], late_parts)

    @pl.when(ro == 1)
    def _():
        diagonal(6)
        diagonal_x(4)
        arrived(direct_y, direct_x, late_parts_less)

    sent = bbuf.at[:, pl.ds(0, 15 * k_half // 8), :]
    remote(sent, sent, send, p_recv.at[0], to_p).wait_send()


def _write(abuf, bbuf, c_ref, o_ref, last, sem):
    co = lax.axis_index("co")
    rows, half = c_ref.shape[1:]
    n = rows // ROWS
    near = pl.multiple_of(co * half, half)
    far = pl.multiple_of((1 - co) * half, half)

    tail = half - LAST

    def write(src, block, cols):
        return pltpu.make_async_copy(src, o_ref.at[block, cols], sem)

    ready = []
    for i in range(2):
        block = pl.ds(i * rows // 2, rows // 2)
        ready.append(write(c_ref.at[0, block, :], block, pl.ds(near, half)))
        ready.append(write(c_ref.at[1, block, pl.ds(0, LAST)], block, pl.ds(far, LAST)))

    def last_out(r):
        block = pl.ds(pl.multiple_of(r * ROWS, ROWS), ROWS)
        return write(last.at[block, :], block, pl.ds(pl.multiple_of(far + LAST, W), tail))

    for copy in ready:
        copy.start()

    @pl.loop(0, n)
    def _(r):
        block = pl.ds(pl.multiple_of(r * ROWS, ROWS), ROWS)
        c = jnp.dot(abuf[block, :], bbuf[1, :, LAST:], preferred_element_type=jnp.float32)
        last[block, :] = c.astype(last.dtype)
        last_out(r).start()

    pltpu.make_async_copy(c_ref, c_ref, sem).wait()


def solution(mesh):
    def local_block(act_blk, weight_blk):
        rows, k = act_blk.shape[0] // 2, act_blk.shape[1] * 2
        half = weight_blk.shape[1]
        dma = pltpu.SemaphoreType.DMA
        vmem = pl.BlockSpec(memory_space=pltpu.VMEM)
        hbm = pl.BlockSpec(memory_space=pl.ANY)
        gathered = pl.pallas_call(
            _gather,
            out_shape=(
                pltpu.VMEM((rows, k), jnp.bfloat16),
                pltpu.VMEM((2, k, half), jnp.bfloat16),
                pltpu.VMEM((2, rows, half), jnp.bfloat16),
            ),
            in_specs=[hbm, hbm],
            out_specs=(vmem, vmem, vmem),
            scratch_shapes=[
                dma,
                dma((2 + len(OWN) + len(VIA_X),)),
                dma((2 + len(sum(VIA_Y, ())),)),
                dma((6,)),
                dma,
            ],
            compiler_params=pltpu.CompilerParams(
                collective_id=0, has_side_effects=True, vmem_limit_bytes=8 * 2**20
            ),
        )(
            pltpu.with_memory_space_constraint(act_blk, pltpu.HBM),
            pltpu.with_memory_space_constraint(weight_blk, pltpu.HBM),
        )
        return pl.pallas_call(
            _write,
            out_shape=jax.ShapeDtypeStruct((rows, 2 * half), jnp.bfloat16),
            in_specs=[vmem, vmem, vmem],
            out_specs=hbm,
            scratch_shapes=[pltpu.VMEM((rows, half - LAST), jnp.bfloat16), dma],
            compiler_params=pltpu.CompilerParams(vmem_limit_bytes=8 * 2**20),
        )(*(pltpu.with_memory_space_constraint(x, pltpu.VMEM) for x in gathered))

    return jax.shard_map(
        local_block,
        mesh=mesh,
        in_specs=(P(("dp", "ro", "ri"), "co"), P(("ro", "ri"), "co")),
        out_specs=P(("dp", "ro", "ri", "co"), None),
        check_vma=False,
    )
```

```python
import functools

import jax
import jax.numpy as jnp
from jax import lax
from jax.experimental import pallas as pl
from jax.experimental.pallas import tpu as pltpu
from jax.sharding import PartitionSpec as P

MESH = pl.DeviceIdType.MESH
W = 256
ROWS = 256
OWN = ((0, 2048), (2048, 1280), (3328, 768))
VIA_Y = (
    ((0, 1024), (1024, 1024)),
    ((2048, 512),),
    ((3328, 256), (3584, 128), (3712, 128)),
)
VIA_X = ((2560, 512), (3072, 256), (3840, 128), (3968, 128))
LAST = 3328


def _gather(a_ref, b_ref, abuf, bbuf, c_ref, send, x_recv, y_recv, p_recv, l_sem):
    ri, co, ro = lax.axis_index("ri"), lax.axis_index("co"), lax.axis_index("ro")
    to_x, to_y, to_p = {"co": 1 - co}, {"ri": 1 - ri}, {"ro": 1 - ro}
    depth, half = b_ref.shape
    rows, k_half = a_ref.shape[0] // 2, a_ref.shape[1]

    mine = (ro * 2 + ri) * depth
    other = (ro * 2 + 1 - ri) * depth
    a_cols = pl.ds(pl.multiple_of(co * k_half, k_half), k_half)

    def remote(src, dst, send, recv, to):
        return pltpu.make_async_remote_copy(
            src_ref=src, dst_ref=dst, send_sem=send, recv_sem=recv, device_id=to, device_id_type=MESH
        )

    def over_x(src, dst, i):
        return remote(src, dst, send, x_recv.at[i], to_x)

    def over_y(src, dst, i):
        return remote(src, dst, send, y_recv.at[i], to_y)

    def over_p(src, dst, i):
        return remote(src, dst, send, p_recv.at[i], to_p)


    def cut(h, block, piece):
        start, size, r0, r1 = (*piece, 0, depth)[:4] if len(piece) == 2 else piece
        return bbuf.at[h, pl.ds(pl.multiple_of(block + r0, 64), r1 - r0), pl.ds(start, size)]
    a_out = over_x(a_ref.at[pl.ds(pl.multiple_of((1 - co) * rows, rows), rows), :], abuf.at[:, a_cols], 0)
    a_loc = pltpu.make_async_copy(
        a_ref.at[pl.ds(pl.multiple_of(co * rows, rows), rows), :], abuf.at[:, a_cols], l_sem
    )
    b_loc = pltpu.make_async_copy(b_ref, cut(0, mine, (0, half)), l_sem)
    loaded = bbuf.at[0, pl.ds(0, 3 * k_half // 4), :]
    n = len(OWN)
    x_own = [over_x(b_ref.at[:, pl.ds(*p)], cut(1, mine, p), 1 + i) for i, p in enumerate(OWN)]
    x_rel = [over_x(cut(0, other, p), cut(1, other, p), 1 + n + i) for i, p in enumerate(VIA_X)]
    direct_x = remote(
        cut(0, other, VIA_X[-1]),
        cut(1, other, VIA_X[-1]),
        send,
        x_recv.at[1 + n + len(VIA_X)],
        {"co": 1 - co, "ro": 1 - ro},
    )
    via_y = sum(VIA_Y, ())
    direct_y = remote(
        cut(1, mine, via_y[-1]),
        cut(1, mine, via_y[-1]),
        send,
        y_recv.at[1 + len(via_y)],
        {"ri": 1 - ri, "ro": 1 - ro},
    )
    y_own = over_y(b_ref, cut(0, mine, (0, half)), 0)
    y_rel = [over_y(cut(1, mine, p), cut(1, mine, p), 1 + i) for i, p in enumerate(via_y)]

    p_own = over_p(b_ref, cut(0, mine, (0, half)), 0)
    p_y = over_p(cut(0, other, (0, half)), cut(0, other, (0, half)), 0)
    p_x = [over_p(cut(1, mine, p), cut(1, mine, p), i) for p, i in zip(OWN, (2, 4, 1))]
    p_dy = [over_p(cut(1, other, p), cut(1, other, p), i) for p, i in zip(via_y, (2, 3, 4, 1, 1, 1))]
    p_dx = [over_p(cut(1, other, p), cut(1, other, p), i) for p, i in zip(VIA_X, (4, 5, 1, 1))]
    near_half = over_p(bbuf.at[0, pl.ds(0, 2 * depth), :], bbuf.at[0, pl.ds(0, 2 * depth), :], 0)

    def both(cols, i):
        rows_in_all = pl.ds(0, cols * depth // half)
        return over_p(bbuf.at[0, rows_in_all, :], bbuf.at[0, rows_in_all, :], i)

    late_parts = both(2 * (half - LAST), 1)
    less = bbuf.at[0, pl.ds(0, 160), pl.ds(0, 4096)]
    late_parts_less = over_p(less, less, 1)
    first_parts = both(2048 + 1024, 2)
    next_parts = both(1280 + 512 + 512, 4)

    barrier = pltpu.get_barrier_semaphore()
    for to in (to_x, to_y, to_p):
        pl.semaphore_signal(barrier, inc=1, device_id=to, device_id_type=MESH)
    pl.semaphore_wait(barrier, 3)

    x_own[0].start()
    y_own.start()
    a_out.start()
    for copy in x_own[1:]:
        copy.start()
    b_loc.start()
    a_loc.start()
    p_own.start()

    def from_y():
        y_own.wait_recv()
        p_y.start()
        for copy in x_rel:
            copy.start()
        pl.when(ro == 0)(direct_x.start)

    def from_x(i):
        x_own[i].wait_recv()
        p_x[i].start()
        first = sum(len(parts) for parts in VIA_Y[:i])
        for copy in y_rel[first : first + len(VIA_Y[i])]:
            copy.start()
        if i == len(VIA_Y) - 1:
            pl.when(ro == 0)(direct_y.start)

    def diagonal(i):
        y_rel[i].wait_recv()
        p_dy[i].start()

    def diagonal_x(i):
        x_rel[i].wait_recv()
        p_dx[i].start()

    def arrived(*copies):
        for copy in copies:
            copy.wait_recv()

    def before(step):
        if step == 0:
            from_x(0)
            from_y()
            pltpu.make_async_copy(loaded, loaded, l_sem).wait()
            arrived(a_out, near_half)
        elif step == 12:
            diagonal(0)
        elif step == 16:
            from_x(1)
            arrived(first_parts)
        elif step == 20:
            from_x(2)
            diagonal(1)
            arrived(p_dy[1])
        elif step == 24:
            diagonal(2)
            diagonal_x(0)
            arrived(next_parts)
        elif step == 27:
            diagonal(3)
            diagonal_x(1)
        elif step == 28:
            arrived(p_dx[1])

    @pl.loop(0, (half + LAST) // W)
    def _(step):
        for at in (0, 12, 16, 20, 24, 27, 28):
            pl.when(step == at)(functools.partial(before, at))
        h = step // (half // W)
        cols = pl.ds(pl.multiple_of(step * W - h * half, W), W)
        c = jnp.dot(abuf[...], bbuf[h, :, cols], preferred_element_type=jnp.float32)
        c_ref[h, :, cols] = c.astype(c_ref.dtype)

    for i in (4,):
        diagonal(i)
        diagonal_x(i - 2)

    @pl.when(ro == 0)
    def _():
        arrived(y_rel[5], x_rel[3], late_parts)

    @pl.when(ro == 1)
    def _():
        diagonal(5)
        diagonal_x(3)
        arrived(direct_y, direct_x, late_parts_less)

    sent = bbuf.at[:, pl.ds(0, 15 * k_half // 8), :]
    remote(sent, sent, send, p_recv.at[0], to_p).wait_send()


def _write(abuf, bbuf, c_ref, o_ref, last, sem):
    co = lax.axis_index("co")
    rows, half = c_ref.shape[1:]
    n = rows // ROWS
    near = pl.multiple_of(co * half, half)
    far = pl.multiple_of((1 - co) * half, half)

    tail = half - LAST

    def write(src, block, cols):
        return pltpu.make_async_copy(src, o_ref.at[block, cols], sem)

    ready = []
    for i in range(2):
        block = pl.ds(i * rows // 2, rows // 2)
        ready.append(write(c_ref.at[0, block, :], block, pl.ds(near, half)))
        ready.append(write(c_ref.at[1, block, pl.ds(0, LAST)], block, pl.ds(far, LAST)))

    def last_out(r):
        block = pl.ds(pl.multiple_of(r * ROWS, ROWS), ROWS)
        return write(last.at[block, :], block, pl.ds(pl.multiple_of(far + LAST, W), tail))

    for copy in ready:
        copy.start()

    @pl.loop(0, n)
    def _(r):
        block = pl.ds(pl.multiple_of(r * ROWS, ROWS), ROWS)
        c = jnp.dot(abuf[block, :], bbuf[1, :, LAST:], preferred_element_type=jnp.float32)
        last[block, :] = c.astype(last.dtype)
        last_out(r).start()

    pltpu.make_async_copy(c_ref, c_ref, sem).wait()


def solution(mesh):
    def local_block(act_blk, weight_blk):
        rows, k = act_blk.shape[0] // 2, act_blk.shape[1] * 2
        half = weight_blk.shape[1]
        dma = pltpu.SemaphoreType.DMA
        vmem = pl.BlockSpec(memory_space=pltpu.VMEM)
        hbm = pl.BlockSpec(memory_space=pl.ANY)
        gathered = pl.pallas_call(
            _gather,
            out_shape=(
                pltpu.VMEM((rows, k), jnp.bfloat16),
                pltpu.VMEM((2, k, half), jnp.bfloat16),
                pltpu.VMEM((2, rows, half), jnp.bfloat16),
            ),
            in_specs=[hbm, hbm],
            out_specs=(vmem, vmem, vmem),
            scratch_shapes=[
                dma,
                dma((2 + len(OWN) + len(VIA_X),)),
                dma((2 + len(sum(VIA_Y, ())),)),
                dma((6,)),
                dma,
            ],
            compiler_params=pltpu.CompilerParams(
                collective_id=0, has_side_effects=True, vmem_limit_bytes=8 * 2**20
            ),
        )(
            pltpu.with_memory_space_constraint(act_blk, pltpu.HBM),
            pltpu.with_memory_space_constraint(weight_blk, pltpu.HBM),
        )
        return pl.pallas_call(
            _write,
            out_shape=jax.ShapeDtypeStruct((rows, 2 * half), jnp.bfloat16),
            in_specs=[vmem, vmem, vmem],
            out_specs=hbm,
            scratch_shapes=[pltpu.VMEM((rows, half - LAST), jnp.bfloat16), dma],
            compiler_params=pltpu.CompilerParams(vmem_limit_bytes=8 * 2**20),
        )(*(pltpu.with_memory_space_constraint(x, pltpu.VMEM) for x in gathered))

    return jax.shard_map(
        local_block,
        mesh=mesh,
        in_specs=(P(("dp", "ro", "ri"), "co"), P(("ro", "ri"), "co")),
        out_specs=P(("dp", "ro", "ri", "co"), None),
        check_vma=False,
    )
```

```python
import functools

import jax
import jax.numpy as jnp
from jax import lax
from jax.experimental import pallas as pl
from jax.experimental.pallas import tpu as pltpu
from jax.sharding import PartitionSpec as P

MESH = pl.DeviceIdType.MESH
W = 256
ROWS = 256
OWN = ((0, 2048), (2048, 1280), (3328, 768))
VIA_Y = (
    ((0, 1024), (1024, 1024)),
    ((2048, 512),),
    ((3328, 256), (3584, 128), (3712, 128)),
)
VIA_X = ((2560, 512), (3072, 256), (3840, 128), (3968, 128))
LAST = 3328


def _gather(a_ref, b_ref, abuf, bbuf, c_ref, send, x_recv, y_recv, p_recv):
    ri, co, ro = lax.axis_index("ri"), lax.axis_index("co"), lax.axis_index("ro")
    to_x, to_y, to_p = {"co": 1 - co}, {"ri": 1 - ri}, {"ro": 1 - ro}
    depth, half = b_ref.shape
    rows, k_half = a_ref.shape[0] // 2, a_ref.shape[1]

    mine = (ro * 2 + ri) * depth
    other = (ro * 2 + 1 - ri) * depth
    a_cols = pl.ds(pl.multiple_of(co * k_half, k_half), k_half)

    def remote(src, dst, send, recv, to):
        return pltpu.make_async_remote_copy(
            src_ref=src, dst_ref=dst, send_sem=send, recv_sem=recv, device_id=to, device_id_type=MESH
        )

    def over_x(src, dst, i):
        return remote(src, dst, send, x_recv.at[i], to_x)

    def over_y(src, dst, i):
        return remote(src, dst, send, y_recv.at[i], to_y)

    def over_p(src, dst, i):
        return remote(src, dst, send, p_recv.at[i], to_p)


    def cut(h, block, piece):
        start, size, r0, r1 = (*piece, 0, depth)[:4] if len(piece) == 2 else piece
        return bbuf.at[h, pl.ds(pl.multiple_of(block + r0, 64), r1 - r0), pl.ds(start, size)]
    a_out = remote(
        a_ref.at[pl.ds(pl.multiple_of((1 - co) * rows, rows), rows), :], abuf.at[:, a_cols], send, p_recv.at[0], to_x
    )
    a_loc = pltpu.make_async_copy(
        a_ref.at[pl.ds(pl.multiple_of(co * rows, rows), rows), :], abuf.at[:, a_cols], p_recv.at[0]
    )
    b_loc = pltpu.make_async_copy(b_ref, cut(0, mine, (0, half)), p_recv.at[0])
    n = len(OWN)
    x_own = [over_x(b_ref.at[:, pl.ds(*p)], cut(1, mine, p), i) for i, p in enumerate(OWN)]
    x_rel = [over_x(cut(0, other, p), cut(1, other, p), n + i) for i, p in enumerate(VIA_X)]
    direct_x = remote(
        cut(0, other, VIA_X[-1]),
        cut(1, other, VIA_X[-1]),
        send,
        p_recv.at[1],
        {"co": 1 - co, "ro": 1 - ro},
    )
    via_y = sum(VIA_Y, ())
    direct_y = remote(
        cut(1, mine, via_y[-1]),
        cut(1, mine, via_y[-1]),
        send,
        p_recv.at[1],
        {"ri": 1 - ri, "ro": 1 - ro},
    )
    y_own = over_y(b_ref, cut(0, mine, (0, half)), 0)
    y_rel = [over_y(cut(1, mine, p), cut(1, mine, p), 1 + i) for i, p in enumerate(via_y)]

    p_own = over_p(b_ref, cut(0, mine, (0, half)), 0)
    p_y = over_p(cut(0, other, (0, half)), cut(0, other, (0, half)), 0)
    p_x = [over_p(cut(1, mine, p), cut(1, mine, p), i) for p, i in zip(OWN, (2, 4, 1))]
    p_dy = [over_p(cut(1, other, p), cut(1, other, p), i) for p, i in zip(via_y, (2, 3, 4, 1, 1, 1))]
    p_dx = [over_p(cut(1, other, p), cut(1, other, p), i) for p, i in zip(VIA_X, (4, 5, 1, 1))]
    near_half = over_p(bbuf.at[0], bbuf.at[0], 0)

    def both(cols, i):
        rows_in_all = pl.ds(0, cols * depth // half)
        return over_p(bbuf.at[0, rows_in_all, :], bbuf.at[0, rows_in_all, :], i)

    late_parts = both(2 * (half - LAST), 1)
    first_parts = both(2048 + 1024, 2)
    next_parts = both(1280 + 512 + 512, 4)

    barrier = pltpu.get_barrier_semaphore()
    for to in (to_x, to_y, to_p):
        pl.semaphore_signal(barrier, inc=1, device_id=to, device_id_type=MESH)
    pl.semaphore_wait(barrier, 3)

    x_own[0].start()
    y_own.start()
    a_out.start()
    for copy in x_own[1:]:
        copy.start()
    b_loc.start()
    a_loc.start()
    p_own.start()

    def from_y():
        y_own.wait_recv()
        p_y.start()
        for copy in x_rel:
            copy.start()
        pl.when(ro == 0)(direct_x.start)

    def from_x(i):
        x_own[i].wait_recv()
        p_x[i].start()
        first = sum(len(parts) for parts in VIA_Y[:i])
        for copy in y_rel[first : first + len(VIA_Y[i])]:
            copy.start()
        if i == len(VIA_Y) - 1:
            pl.when(ro == 0)(direct_y.start)

    def diagonal(i):
        y_rel[i].wait_recv()
        p_dy[i].start()

    def diagonal_x(i):
        x_rel[i].wait_recv()
        p_dx[i].start()

    def arrived(*copies):
        for copy in copies:
            copy.wait_recv()

    def before(step):
        if step == 0:
            from_x(0)
            from_y()
            arrived(near_half)
        elif step == 12:
            diagonal(0)
        elif step == 16:
            from_x(1)
            arrived(first_parts)
        elif step == 20:
            from_x(2)
            diagonal(1)
            arrived(p_dy[1])
        elif step == 24:
            diagonal(2)
            diagonal_x(0)
            arrived(next_parts)
        elif step == 27:
            diagonal(3)
            diagonal_x(1)
        elif step == 28:
            arrived(p_dx[1])

    @pl.loop(0, (half + LAST) // W)
    def _(step):
        for at in (0, 12, 16, 20, 24, 27, 28):
            pl.when(step == at)(functools.partial(before, at))
        h = step // (half // W)
        cols = pl.ds(pl.multiple_of(step * W - h * half, W), W)
        c = jnp.dot(abuf[...], bbuf[h, :, cols], preferred_element_type=jnp.float32)
        c_ref[h, :, cols] = c.astype(c_ref.dtype)

    for i in (4,):
        diagonal(i)
        diagonal_x(i - 2)

    y_rel[5].wait_recv()
    x_rel[3].wait_recv()

    @pl.when(ro == 1)
    def _():
        p_dy[5].start()
        p_dx[3].start()

    arrived(late_parts)

    sent = bbuf.at[:, pl.ds(0, 15 * k_half // 8), :]
    remote(sent, sent, send, p_recv.at[0], to_p).wait_send()


def _write(abuf, bbuf, c_ref, o_ref, last, sem):
    co = lax.axis_index("co")
    rows, half = c_ref.shape[1:]
    n = rows // ROWS
    near = pl.multiple_of(co * half, half)
    far = pl.multiple_of((1 - co) * half, half)

    tail = half - LAST

    def write(src, block, cols):
        return pltpu.make_async_copy(src, o_ref.at[block, cols], sem)

    ready = []
    for i in range(2):
        block = pl.ds(i * rows // 2, rows // 2)
        ready.append(write(c_ref.at[0, block, :], block, pl.ds(near, half)))
        ready.append(write(c_ref.at[1, block, pl.ds(0, LAST)], block, pl.ds(far, LAST)))

    def last_out(r):
        block = pl.ds(pl.multiple_of(r * ROWS, ROWS), ROWS)
        return write(last.at[block, :], block, pl.ds(pl.multiple_of(far + LAST, W), tail))

    for copy in ready:
        copy.start()

    @pl.loop(0, n)
    def _(r):
        block = pl.ds(pl.multiple_of(r * ROWS, ROWS), ROWS)
        c = jnp.dot(abuf[block, :], bbuf[1, :, LAST:], preferred_element_type=jnp.float32)
        last[block, :] = c.astype(last.dtype)
        last_out(r).start()

    pltpu.make_async_copy(c_ref, c_ref, sem).wait()


def solution(mesh):
    def local_block(act_blk, weight_blk):
        rows, k = act_blk.shape[0] // 2, act_blk.shape[1] * 2
        half = weight_blk.shape[1]
        dma = pltpu.SemaphoreType.DMA
        vmem = pl.BlockSpec(memory_space=pltpu.VMEM)
        hbm = pl.BlockSpec(memory_space=pl.ANY)
        gathered = pl.pallas_call(
            _gather,
            out_shape=(
                pltpu.VMEM((rows, k), jnp.bfloat16),
                pltpu.VMEM((2, k, half), jnp.bfloat16),
                pltpu.VMEM((2, rows, half), jnp.bfloat16),
            ),
            in_specs=[hbm, hbm],
            out_specs=(vmem, vmem, vmem),
            scratch_shapes=[
                dma,
                dma((len(OWN) + len(VIA_X),)),
                dma((1 + len(sum(VIA_Y, ())),)),
                dma((6,)),
            ],
            compiler_params=pltpu.CompilerParams(
                collective_id=0, has_side_effects=True, vmem_limit_bytes=8 * 2**20
            ),
        )(
            pltpu.with_memory_space_constraint(act_blk, pltpu.HBM),
            pltpu.with_memory_space_constraint(weight_blk, pltpu.HBM),
        )
        return pl.pallas_call(
            _write,
            out_shape=jax.ShapeDtypeStruct((rows, 2 * half), jnp.bfloat16),
            in_specs=[vmem, vmem, vmem],
            out_specs=hbm,
            scratch_shapes=[pltpu.VMEM((rows, half - LAST), jnp.bfloat16), dma],
            compiler_params=pltpu.CompilerParams(vmem_limit_bytes=8 * 2**20),
        )(*(pltpu.with_memory_space_constraint(x, pltpu.VMEM) for x in gathered))

    return jax.shard_map(
        local_block,
        mesh=mesh,
        in_specs=(P(("dp", "ro", "ri"), "co"), P(("ro", "ri"), "co")),
        out_specs=P(("dp", "ro", "ri", "co"), None),
        check_vma=False,
    )
```

```python
import functools

import jax
import jax.numpy as jnp
from jax import lax
from jax.experimental import pallas as pl
from jax.experimental.pallas import tpu as pltpu
from jax.sharding import PartitionSpec as P

MESH = pl.DeviceIdType.MESH
W = 256
ROWS = 256
OWN = ((0, 2048), (2048, 1280), (3328, 768))
VIA_Y = (
    ((0, 1024), (1024, 1024)),
    ((2048, 512),),
    ((3328, 256), (3584, 128), (3712, 128)),
)
VIA_X = ((2560, 512), (3072, 256), (3840, 128), (3968, 128))
LAST = 3328


def _gather(a_ref, b_ref, abuf, bbuf, c_ref, send, recv, p_recv):
    ri, co, ro = lax.axis_index("ri"), lax.axis_index("co"), lax.axis_index("ro")
    to_x, to_y, to_p = {"co": 1 - co}, {"ri": 1 - ri}, {"ro": 1 - ro}
    depth, half = b_ref.shape
    rows, k_half = a_ref.shape[0] // 2, a_ref.shape[1]

    mine = (ro * 2 + ri) * depth
    other = (ro * 2 + 1 - ri) * depth
    a_cols = pl.ds(pl.multiple_of(co * k_half, k_half), k_half)

    def remote(src, dst, send, recv, to):
        return pltpu.make_async_remote_copy(
            src_ref=src, dst_ref=dst, send_sem=send, recv_sem=recv, device_id=to, device_id_type=MESH
        )

    def over_x(src, dst, i):
        return remote(src, dst, send, recv.at[i], to_x)

    def over_y(src, dst, i):
        return remote(src, dst, send, recv.at[i], to_y)

    def over_p(src, dst, i):
        return remote(src, dst, send, p_recv.at[i], to_p)


    def cut(h, block, piece):
        start, size, r0, r1 = (*piece, 0, depth)[:4] if len(piece) == 2 else piece
        return bbuf.at[h, pl.ds(pl.multiple_of(block + r0, 64), r1 - r0), pl.ds(start, size)]
    a_out = remote(
        a_ref.at[pl.ds(pl.multiple_of((1 - co) * rows, rows), rows), :], abuf.at[:, a_cols], send, p_recv.at[0], to_x
    )
    a_loc = pltpu.make_async_copy(
        a_ref.at[pl.ds(pl.multiple_of(co * rows, rows), rows), :], abuf.at[:, a_cols], p_recv.at[0]
    )
    b_loc = pltpu.make_async_copy(b_ref, cut(0, mine, (0, half)), p_recv.at[0])
    n = len(OWN)
    x_own = [over_x(b_ref.at[:, pl.ds(*p)], cut(1, mine, p), i) for i, p in enumerate(OWN)]
    x_rel = [over_x(cut(0, other, p), cut(1, other, p), i) for p, i in zip(VIA_X, (5, 6, 7, 8))]
    direct_x = remote(
        cut(0, other, VIA_X[-1]),
        cut(1, other, VIA_X[-1]),
        send,
        p_recv.at[1],
        {"co": 1 - co, "ro": 1 - ro},
    )
    via_y = sum(VIA_Y, ())
    direct_y = remote(
        cut(1, mine, via_y[-1]),
        cut(1, mine, via_y[-1]),
        send,
        p_recv.at[1],
        {"ri": 1 - ri, "ro": 1 - ro},
    )
    y_own = over_y(b_ref, cut(0, mine, (0, half)), 3)
    y_rel = [over_y(cut(1, mine, p), cut(1, mine, p), i) for p, i in zip(via_y, (4, 2, 5, 6, 7, 8))]

    p_own = over_p(b_ref, cut(0, mine, (0, half)), 0)
    p_y = over_p(cut(0, other, (0, half)), cut(0, other, (0, half)), 0)
    p_x = [over_p(cut(1, mine, p), cut(1, mine, p), i) for p, i in zip(OWN, (2, 4, 1))]
    p_dy = [over_p(cut(1, other, p), cut(1, other, p), i) for p, i in zip(via_y, (2, 3, 4, 1, 1, 1))]
    p_dx = [over_p(cut(1, other, p), cut(1, other, p), i) for p, i in zip(VIA_X, (4, 5, 1, 1))]
    near_half = over_p(bbuf.at[0], bbuf.at[0], 0)

    def both(cols, i):
        rows_in_all = pl.ds(0, cols * depth // half)
        return over_p(bbuf.at[0, rows_in_all, :], bbuf.at[0, rows_in_all, :], i)

    late_parts = both(2 * (half - LAST), 1)
    first_parts = both(2048 + 1024, 2)
    next_parts = both(1280 + 512 + 512, 4)

    barrier = pltpu.get_barrier_semaphore()
    for to in (to_x, to_y, to_p):
        pl.semaphore_signal(barrier, inc=1, device_id=to, device_id_type=MESH)
    pl.semaphore_wait(barrier, 3)

    x_own[0].start()
    y_own.start()
    a_out.start()
    for copy in x_own[1:]:
        copy.start()
    b_loc.start()
    a_loc.start()
    p_own.start()

    def from_y():
        y_own.wait_recv()
        p_y.start()
        for copy in x_rel:
            copy.start()
        pl.when(ro == 0)(direct_x.start)

    def came(cols, i):
        part = bbuf.at[0, pl.ds(0, cols * depth // half), :]
        remote(part, part, send, recv.at[i], to_p).wait_recv()

    def pass_on(i):
        p_x[i].start()
        first = sum(len(parts) for parts in VIA_Y[:i])
        for copy in y_rel[first : first + len(VIA_Y[i])]:
            copy.start()
        if i == len(VIA_Y) - 1:
            pl.when(ro == 0)(direct_y.start)

    def from_x(i):
        x_own[i].wait_recv()
        pass_on(i)

    def diagonal(i):
        came(via_y[i][1] + VIA_X[i - 2][1], i + 3)
        p_dy[i].start()
        p_dx[i - 2].start()

    def arrived(*copies):
        for copy in copies:
            copy.wait_recv()

    def before(step):
        if step == 0:
            from_x(0)
            from_y()
            arrived(near_half)
        elif step == 12:
            y_rel[0].wait_recv()
            p_dy[0].start()
        elif step == 16:
            from_x(1)
            arrived(first_parts)
        elif step == 20:
            came(OWN[2][1] + via_y[1][1], 2)
            pass_on(2)
            p_dy[1].start()
            arrived(p_dy[1])
        elif step == 24:
            diagonal(2)
            arrived(next_parts)
        elif step == 27:
            diagonal(3)
        elif step == 28:
            arrived(p_dx[1])

    @pl.loop(0, (half + LAST) // W)
    def _(step):
        for at in (0, 12, 16, 20, 24, 27, 28):
            pl.when(step == at)(functools.partial(before, at))
        h = step // (half // W)
        cols = pl.ds(pl.multiple_of(step * W - h * half, W), W)
        c = jnp.dot(abuf[...], bbuf[h, :, cols], preferred_element_type=jnp.float32)
        c_ref[h, :, cols] = c.astype(c_ref.dtype)

    diagonal(4)

    came(via_y[5][1] + VIA_X[3][1], 8)

    @pl.when(ro == 1)
    def _():
        p_dy[5].start()
        p_dx[3].start()

    arrived(late_parts)

    sent = bbuf.at[:, pl.ds(0, 15 * k_half // 8), :]
    remote(sent, sent, send, p_recv.at[0], to_p).wait_send()


def _write(abuf, bbuf, c_ref, o_ref, last, sem):
    co = lax.axis_index("co")
    rows, half = c_ref.shape[1:]
    n = rows // ROWS
    near = pl.multiple_of(co * half, half)
    far = pl.multiple_of((1 - co) * half, half)

    tail = half - LAST

    def write(src, block, cols):
        return pltpu.make_async_copy(src, o_ref.at[block, cols], sem)

    ready = []
    for i in range(2):
        block = pl.ds(i * rows // 2, rows // 2)
        ready.append(write(c_ref.at[0, block, :], block, pl.ds(near, half)))
        ready.append(write(c_ref.at[1, block, pl.ds(0, LAST)], block, pl.ds(far, LAST)))

    def last_out(r):
        block = pl.ds(pl.multiple_of(r * ROWS, ROWS), ROWS)
        return write(last.at[block, :], block, pl.ds(pl.multiple_of(far + LAST, W), tail))

    for copy in ready:
        copy.start()

    @pl.loop(0, n)
    def _(r):
        block = pl.ds(pl.multiple_of(r * ROWS, ROWS), ROWS)
        c = jnp.dot(abuf[block, :], bbuf[1, :, LAST:], preferred_element_type=jnp.float32)
        last[block, :] = c.astype(last.dtype)
        last_out(r).start()

    pltpu.make_async_copy(c_ref, c_ref, sem).wait()


def solution(mesh):
    def local_block(act_blk, weight_blk):
        rows, k = act_blk.shape[0] // 2, act_blk.shape[1] * 2
        half = weight_blk.shape[1]
        dma = pltpu.SemaphoreType.DMA
        vmem = pl.BlockSpec(memory_space=pltpu.VMEM)
        hbm = pl.BlockSpec(memory_space=pl.ANY)
        gathered = pl.pallas_call(
            _gather,
            out_shape=(
                pltpu.VMEM((rows, k), jnp.bfloat16),
                pltpu.VMEM((2, k, half), jnp.bfloat16),
                pltpu.VMEM((2, rows, half), jnp.bfloat16),
            ),
            in_specs=[hbm, hbm],
            out_specs=(vmem, vmem, vmem),
            scratch_shapes=[
                dma,
                dma((9,)),
                dma((6,)),
            ],
            compiler_params=pltpu.CompilerParams(
                collective_id=0, has_side_effects=True, vmem_limit_bytes=8 * 2**20
            ),
        )(
            pltpu.with_memory_space_constraint(act_blk, pltpu.HBM),
            pltpu.with_memory_space_constraint(weight_blk, pltpu.HBM),
        )
        return pl.pallas_call(
            _write,
            out_shape=jax.ShapeDtypeStruct((rows, 2 * half), jnp.bfloat16),
            in_specs=[vmem, vmem, vmem],
            out_specs=hbm,
            scratch_shapes=[pltpu.VMEM((rows, half - LAST), jnp.bfloat16), dma],
            compiler_params=pltpu.CompilerParams(vmem_limit_bytes=8 * 2**20),
        )(*(pltpu.with_memory_space_constraint(x, pltpu.VMEM) for x in gathered))

    return jax.shard_map(
        local_block,
        mesh=mesh,
        in_specs=(P(("dp", "ro", "ri"), "co"), P(("ro", "ri"), "co")),
        out_specs=P(("dp", "ro", "ri", "co"), None),
        check_vma=False,
    )
```

```python
import functools

import jax
import jax.numpy as jnp
from jax import lax
from jax.experimental import pallas as pl
from jax.experimental.pallas import tpu as pltpu
from jax.sharding import PartitionSpec as P

MESH = pl.DeviceIdType.MESH
W = 256
ROWS = 256
OWN = ((0, 2048), (2048, 1280), (3328, 768))
VIA_Y = (
    ((0, 1024), (1024, 1024)),
    ((2048, 512),),
    ((3328, 256), (3584, 128), (3712, 128)),
)
VIA_X = ((2560, 512), (3072, 256), (3840, 128), (3968, 128))
LAST = 3328


def _gather(a_ref, b_ref, abuf, bbuf, c_ref, send, recv, p_recv):
    ri, co, ro = lax.axis_index("ri"), lax.axis_index("co"), lax.axis_index("ro")
    to_x, to_y, to_p = {"co": 1 - co}, {"ri": 1 - ri}, {"ro": 1 - ro}
    depth, half = b_ref.shape
    rows, k_half = a_ref.shape[0] // 2, a_ref.shape[1]

    mine = (ro * 2 + ri) * depth
    other = (ro * 2 + 1 - ri) * depth
    a_cols = pl.ds(pl.multiple_of(co * k_half, k_half), k_half)

    def remote(src, dst, send, recv, to):
        return pltpu.make_async_remote_copy(
            src_ref=src, dst_ref=dst, send_sem=send, recv_sem=recv, device_id=to, device_id_type=MESH
        )

    def over_x(src, dst, i):
        return remote(src, dst, send, recv.at[i], to_x)

    def over_y(src, dst, i):
        return remote(src, dst, send, recv.at[i], to_y)

    def over_p(src, dst, i):
        return remote(src, dst, send, p_recv.at[i], to_p)


    def cut(h, block, piece):
        start, size, r0, r1 = (*piece, 0, depth)[:4] if len(piece) == 2 else piece
        return bbuf.at[h, pl.ds(pl.multiple_of(block + r0, 64), r1 - r0), pl.ds(start, size)]
    a_out = remote(
        a_ref.at[pl.ds(pl.multiple_of((1 - co) * rows, rows), rows), :], abuf.at[:, a_cols], send, p_recv.at[0], to_x
    )
    a_loc = pltpu.make_async_copy(
        a_ref.at[pl.ds(pl.multiple_of(co * rows, rows), rows), :], abuf.at[:, a_cols], p_recv.at[0]
    )
    b_loc = pltpu.make_async_copy(b_ref, cut(0, mine, (0, half)), p_recv.at[0])
    n = len(OWN)
    x_own = [over_x(b_ref.at[:, pl.ds(*p)], cut(1, mine, p), i) for i, p in enumerate(OWN)]
    x_rel = [over_x(cut(0, other, p), cut(1, other, p), i) for p, i in zip(VIA_X, (4, 5, 6, 7))]
    direct_x = remote(
        cut(0, other, VIA_X[-1]),
        cut(1, other, VIA_X[-1]),
        send,
        p_recv.at[1],
        {"co": 1 - co, "ro": 1 - ro},
    )
    via_y = sum(VIA_Y, ())
    direct_y = remote(
        cut(1, mine, via_y[-1]),
        cut(1, mine, via_y[-1]),
        send,
        p_recv.at[1],
        {"ri": 1 - ri, "ro": 1 - ro},
    )
    y_own = over_y(b_ref, cut(0, mine, (0, half)), 3)
    y_rel = [over_y(cut(1, mine, p), cut(1, mine, p), i) for p, i in zip(via_y, (1, 2, 4, 5, 6, 7))]

    p_own = over_p(b_ref, cut(0, mine, (0, half)), 0)
    p_y = over_p(cut(0, other, (0, half)), cut(0, other, (0, half)), 0)
    p_x = [over_p(cut(1, mine, p), cut(1, mine, p), i) for p, i in zip(OWN, (2, 4, 1))]
    p_dy = [over_p(cut(1, other, p), cut(1, other, p), i) for p, i in zip(via_y, (2, 3, 4, 1, 1, 1))]
    p_dx = [over_p(cut(1, other, p), cut(1, other, p), i) for p, i in zip(VIA_X, (4, 5, 1, 1))]
    near_half = over_p(bbuf.at[0], bbuf.at[0], 0)

    def both(cols, i):
        rows_in_all = pl.ds(0, cols * depth // half)
        return over_p(bbuf.at[0, rows_in_all, :], bbuf.at[0, rows_in_all, :], i)

    late_parts = both(2 * (half - LAST), 1)
    first_parts = both(2048 + 1024, 2)
    next_parts = both(1280 + 512 + 512, 4)

    barrier = pltpu.get_barrier_semaphore()
    for to in (to_x, to_y, to_p):
        pl.semaphore_signal(barrier, inc=1, device_id=to, device_id_type=MESH)
    pl.semaphore_wait(barrier, 3)

    x_own[0].start()
    y_own.start()
    a_out.start()
    for copy in x_own[1:]:
        copy.start()
    b_loc.start()
    a_loc.start()
    p_own.start()

    def from_y():
        y_own.wait_recv()
        p_y.start()
        for copy in x_rel:
            copy.start()
        pl.when(ro == 0)(direct_x.start)

    def came(cols, i):
        part = bbuf.at[0, pl.ds(0, cols * depth // half), :]
        remote(part, part, send, recv.at[i], to_p).wait_recv()

    def pass_on(i):
        p_x[i].start()
        first = sum(len(parts) for parts in VIA_Y[:i])
        for copy in y_rel[first : first + len(VIA_Y[i])]:
            copy.start()
        if i == len(VIA_Y) - 1:
            pl.when(ro == 0)(direct_y.start)

    def from_x(i):
        x_own[i].wait_recv()
        pass_on(i)

    def diagonal(i):
        came(via_y[i][1] + VIA_X[i - 2][1], i + 2)
        p_dy[i].start()
        p_dx[i - 2].start()

    def arrived(*copies):
        for copy in copies:
            copy.wait_recv()

    def before(step):
        if step == 0:
            from_x(0)
            from_y()
            arrived(near_half)
        elif step == 16:
            came(OWN[1][1] + via_y[0][1], 1)
            pass_on(1)
            p_dy[0].start()
            arrived(first_parts)
        elif step == 20:
            came(OWN[2][1] + via_y[1][1], 2)
            pass_on(2)
            p_dy[1].start()
            arrived(p_dy[1])
        elif step == 24:
            diagonal(2)
            arrived(next_parts)
        elif step == 27:
            diagonal(3)
        elif step == 28:
            arrived(p_dx[1])

    @pl.loop(0, (half + LAST) // W)
    def _(step):
        for at in (0, 16, 20, 24, 27, 28):
            pl.when(step == at)(functools.partial(before, at))
        h = step // (half // W)
        cols = pl.ds(pl.multiple_of(step * W - h * half, W), W)
        c = jnp.dot(abuf[...], bbuf[h, :, cols], preferred_element_type=jnp.float32)
        c_ref[h, :, cols] = c.astype(c_ref.dtype)

    diagonal(4)

    came(via_y[5][1] + VIA_X[3][1], 7)

    @pl.when(ro == 1)
    def _():
        p_dy[5].start()
        p_dx[3].start()

    arrived(late_parts)

    sent = bbuf.at[:, pl.ds(0, 15 * k_half // 8), :]
    remote(sent, sent, send, p_recv.at[0], to_p).wait_send()


def _write(abuf, bbuf, c_ref, o_ref, last, sem):
    co = lax.axis_index("co")
    rows, half = c_ref.shape[1:]
    n = rows // ROWS
    near = pl.multiple_of(co * half, half)
    far = pl.multiple_of((1 - co) * half, half)

    tail = half - LAST

    def write(src, block, cols):
        return pltpu.make_async_copy(src, o_ref.at[block, cols], sem)

    ready = []
    for i in range(2):
        block = pl.ds(i * rows // 2, rows // 2)
        ready.append(write(c_ref.at[0, block, :], block, pl.ds(near, half)))
        ready.append(write(c_ref.at[1, block, pl.ds(0, LAST)], block, pl.ds(far, LAST)))

    def last_out(r):
        block = pl.ds(pl.multiple_of(r * ROWS, ROWS), ROWS)
        return write(last.at[block, :], block, pl.ds(pl.multiple_of(far + LAST, W), tail))

    for copy in ready:
        copy.start()

    @pl.loop(0, n)
    def _(r):
        block = pl.ds(pl.multiple_of(r * ROWS, ROWS), ROWS)
        c = jnp.dot(abuf[block, :], bbuf[1, :, LAST:], preferred_element_type=jnp.float32)
        last[block, :] = c.astype(last.dtype)
        last_out(r).start()

    pltpu.make_async_copy(c_ref, c_ref, sem).wait()


def solution(mesh):
    def local_block(act_blk, weight_blk):
        rows, k = act_blk.shape[0] // 2, act_blk.shape[1] * 2
        half = weight_blk.shape[1]
        dma = pltpu.SemaphoreType.DMA
        vmem = pl.BlockSpec(memory_space=pltpu.VMEM)
        hbm = pl.BlockSpec(memory_space=pl.ANY)
        gathered = pl.pallas_call(
            _gather,
            out_shape=(
                pltpu.VMEM((rows, k), jnp.bfloat16),
                pltpu.VMEM((2, k, half), jnp.bfloat16),
                pltpu.VMEM((2, rows, half), jnp.bfloat16),
            ),
            in_specs=[hbm, hbm],
            out_specs=(vmem, vmem, vmem),
            scratch_shapes=[
                dma,
                dma((8,)),
                dma((6,)),
            ],
            compiler_params=pltpu.CompilerParams(
                collective_id=0, has_side_effects=True, vmem_limit_bytes=8 * 2**20
            ),
        )(
            pltpu.with_memory_space_constraint(act_blk, pltpu.HBM),
            pltpu.with_memory_space_constraint(weight_blk, pltpu.HBM),
        )
        return pl.pallas_call(
            _write,
            out_shape=jax.ShapeDtypeStruct((rows, 2 * half), jnp.bfloat16),
            in_specs=[vmem, vmem, vmem],
            out_specs=hbm,
            scratch_shapes=[pltpu.VMEM((rows, half - LAST), jnp.bfloat16), dma],
            compiler_params=pltpu.CompilerParams(vmem_limit_bytes=8 * 2**20),
        )(*(pltpu.with_memory_space_constraint(x, pltpu.VMEM) for x in gathered))

    return jax.shard_map(
        local_block,
        mesh=mesh,
        in_specs=(P(("dp", "ro", "ri"), "co"), P(("ro", "ri"), "co")),
        out_specs=P(("dp", "ro", "ri", "co"), None),
        check_vma=False,
    )
```
